32 devices in a mesh: dp: 1 (over z), tp: 4 (over y), cp: 8 (over x, core).
Axes of the slice: x: 4, y: 4, z: 1, core: 2. Of those that a mesh axis runs over, the one named last changes fastest.
The devices are a block of a 4x4x8 slice.
Arguments:
- x: bfloat16 [8192, 4096], P(('dp', 'cp'))
- attn_gain: bfloat16 [4096], replicated
- w_q: bfloat16 [4096, 4096], P(None, 'tp')
- w_k: bfloat16 [4096, 1024], P(None, 'tp')
- w_v: bfloat16 [4096, 1024], P(None, 'tp')
- w_o: bfloat16 [4096, 4096], P('tp')
- mlp_gain: bfloat16 [4096], replicated
- w_gate: bfloat16 [4096, 14336], P(None, 'tp')
- w_up: bfloat16 [4096, 14336], P(None, 'tp')
- w_down: bfloat16 [14336, 4096], P('tp')
Outputs:
- output 1: bfloat16 [8192, 4096], P(('dp', 'cp'))
- output 2: bfloat16 [8192, 8, 128], P(('dp', 'cp'), 'tp')
- output 3: bfloat16 [8192, 8, 128], P(('dp', 'cp'), 'tp')
All inputs are finite; a program needn't handle non-finite values.
Results may differ from the reference program's by a relative error of at most 0.013606.
Values are sent between devices in bfloat16 or wider.
A program may use at most 768 MiB of HBM per device.

```python
import jax
import jax.numpy as jnp
from jax import lax

SEQ_LEN = 8192
MODEL_DIM = 4096
FF_DIM = 14336
NUM_HEADS = 32
KV_HEADS = 8
HEAD_DIM = 128
ROPE_THETA = 1000000
BLOCK_LEN = 256
NORM_EPS = 1e-5
MASK_VALUE = -1e30


def setup_inputs(seed: int = 0, part: int = 0) -> dict:
    root = jax.random.key(seed)
    key_list = jax.random.split(root, 10)
    seq_key = jax.random.fold_in(key_list[0], part)
    noise_key, dir_key, freq_key, phase_key = jax.random.split(seq_key, 4)
    seq_frac = jnp.arange(SEQ_LEN, dtype=jnp.float32) / SEQ_LEN
    wave_freq = jax.random.uniform(freq_key, (4,), jnp.float32, 0.3, 2.0)
    wave_phase = jax.random.uniform(phase_key, (4,), jnp.float32, 0.0, 6.2831853)
    waves = jnp.cos(6.2831853 * seq_frac[:, None] * wave_freq[None, :] + wave_phase[None, :])
    directions = 0.5 * jax.random.normal(dir_key, (4, MODEL_DIM), jnp.float32)
    noise = jax.random.normal(noise_key, (SEQ_LEN, MODEL_DIM), jnp.float32)
    x = (0.6 * noise + jnp.dot(waves, directions)).astype(jnp.bfloat16)
    q_cols = NUM_HEADS * HEAD_DIM
    kv_cols = KV_HEADS * HEAD_DIM

    def weight(key, rows, cols):
        return (jax.random.normal(key, (rows, cols), jnp.float32) * rows ** -0.5).astype(jnp.bfloat16)

    def gain(key):
        return jax.random.uniform(key, (MODEL_DIM,), jnp.float32, 0.5, 1.5).astype(jnp.bfloat16)

    return {
        'x': x,
        'attn_gain': gain(key_list[1]),
        'w_q': weight(key_list[2], MODEL_DIM, q_cols),
        'w_k': weight(key_list[3], MODEL_DIM, kv_cols),
        'w_v': weight(key_list[4], MODEL_DIM, kv_cols),
        'w_o': weight(key_list[5], q_cols, MODEL_DIM),
        'mlp_gain': gain(key_list[6]),
        'w_gate': weight(key_list[7], MODEL_DIM, FF_DIM),
        'w_up': weight(key_list[8], MODEL_DIM, FF_DIM),
        'w_down': weight(key_list[9], FF_DIM, MODEL_DIM),
    }


def rms_norm(rows, gain):
    wide = rows.astype(jnp.float32)
    inv_rms = lax.rsqrt(jnp.mean(wide * wide, axis=-1, keepdims=True) + NORM_EPS)
    return (wide * inv_rms * gain.astype(jnp.float32)).astype(jnp.bfloat16)


def rope_tables(positions):
    inv_freq = jnp.asarray(ROPE_THETA, jnp.float32) ** (-jnp.arange(0, HEAD_DIM, 2, dtype=jnp.float32) / HEAD_DIM)
    angles = positions.astype(jnp.float32)[:, None] * inv_freq[None, :]
    return jnp.cos(angles), jnp.sin(angles)


def apply_rope(heads, cos_b, sin_b):
    half = HEAD_DIM // 2
    wide = heads.astype(jnp.float32)
    first = wide[..., :half]
    second = wide[..., half:]
    return jnp.concatenate([first * cos_b - second * sin_b, second * cos_b + first * sin_b], axis=-1).astype(jnp.bfloat16)


def causal_attention(queries, keys, values):
    groups = NUM_HEADS // KV_HEADS
    n_blocks = SEQ_LEN // BLOCK_LEN
    q_blocks = queries.reshape(n_blocks, BLOCK_LEN, KV_HEADS, groups, HEAD_DIM)
    k_blocks = keys.reshape(n_blocks, BLOCK_LEN, KV_HEADS, HEAD_DIM)
    v_blocks = values.reshape(n_blocks, BLOCK_LEN, KV_HEADS, HEAD_DIM)
    offsets = jnp.arange(BLOCK_LEN)
    block_ids = jnp.arange(n_blocks)

    def one_query_block(operands):
        q_blk, q_idx = operands
        q_wide = q_blk.astype(jnp.float32)
        q_pos = q_idx * BLOCK_LEN + offsets

        def key_step(carry, inputs):
            run_max, run_sum, weighted = carry
            k_blk, v_blk, k_idx = inputs
            k_pos = k_idx * BLOCK_LEN + offsets
            scores = jnp.einsum('qkgd,skd->kgqs', q_wide, k_blk.astype(jnp.float32)) * (HEAD_DIM ** -0.5)
            scores = jnp.where(k_pos[None, :] <= q_pos[:, None], scores, MASK_VALUE)
            new_max = jnp.maximum(run_max, jnp.max(scores, axis=-1))
            rescale = jnp.exp(run_max - new_max)
            exp_scores = jnp.exp(scores - new_max[..., None])
            new_sum = run_sum * rescale + jnp.sum(exp_scores, axis=-1)
            exp_rounded = exp_scores.astype(jnp.bfloat16).astype(jnp.float32)
            new_weighted = weighted * rescale[..., None] + jnp.einsum('kgqs,skd->kgqd', exp_rounded, v_blk.astype(jnp.float32))
            return (new_max, new_sum, new_weighted), None

        stat_shape = (KV_HEADS, groups, BLOCK_LEN)
        init = (jnp.full(stat_shape, MASK_VALUE, jnp.float32), jnp.zeros(stat_shape, jnp.float32), jnp.zeros(stat_shape + (HEAD_DIM,), jnp.float32))
        final, unused = lax.scan(key_step, init, (k_blocks, v_blocks, block_ids))
        block_out = final[2] / final[1][..., None]
        return jnp.transpose(block_out, (2, 0, 1, 3)).astype(jnp.bfloat16)

    outs = lax.map(one_query_block, (q_blocks, block_ids))
    return outs.reshape(SEQ_LEN, NUM_HEADS * HEAD_DIM)


def reference(x, attn_gain, w_q, w_k, w_v, w_o, mlp_gain, w_gate, w_up, w_down):
    groups = NUM_HEADS // KV_HEADS
    cos_tab, sin_tab = rope_tables(jnp.arange(SEQ_LEN))
    normed = rms_norm(x, attn_gain)
    queries = jnp.dot(normed, w_q, preferred_element_type=jnp.float32).astype(jnp.bfloat16).reshape(SEQ_LEN, NUM_HEADS, HEAD_DIM)
    keys = jnp.dot(normed, w_k, preferred_element_type=jnp.float32).astype(jnp.bfloat16).reshape(SEQ_LEN, KV_HEADS, HEAD_DIM)
    values = jnp.dot(normed, w_v, preferred_element_type=jnp.float32).astype(jnp.bfloat16).reshape(SEQ_LEN, KV_HEADS, HEAD_DIM)
    queries = apply_rope(queries, cos_tab[:, None, :], sin_tab[:, None, :])
    keys = apply_rope(keys, cos_tab[:, None, :], sin_tab[:, None, :])
    attn_rows = causal_attention(queries.reshape(SEQ_LEN, KV_HEADS, groups, HEAD_DIM), keys, values)
    attn_proj = jnp.dot(attn_rows, w_o, preferred_element_type=jnp.float32)
    hidden = (x.astype(jnp.float32) + attn_proj).astype(jnp.bfloat16)
    normed_mlp = rms_norm(hidden, mlp_gain)
    gate_proj = jnp.dot(normed_mlp, w_gate, preferred_element_type=jnp.float32)
    up_proj = jnp.dot(normed_mlp, w_up, preferred_element_type=jnp.float32)
    activated = (jax.nn.silu(gate_proj) * up_proj).astype(jnp.bfloat16)
    down_proj = jnp.dot(activated, w_down, preferred_element_type=jnp.float32)
    x_out = (hidden.astype(jnp.float32) + down_proj).astype(jnp.bfloat16)
    return (x_out, keys, values)
```

```python
import functools
import math
import jax
import jax.numpy as jnp
from jax import lax
from jax.experimental import pallas as pl
from jax.experimental.pallas import tpu as pltpu
from jax.sharding import PartitionSpec as P

HEAD_DIM = 128
ROPE_THETA = 1000000.0
NORM_EPS = 1e-5
MASK_VALUE = -1e30
SCORE_EXP2 = HEAD_DIM ** -0.5 * math.log2(math.e)
KEY_TILE = 1024
ROW_TILE = 256
COL_TILE = 1024
FF_TILE = 512
VMEM_LIMIT = 60 * 1024 * 1024


def rms_norm(rows, gain):
    wide = rows.astype(jnp.float32)
    inv_rms = lax.rsqrt(jnp.mean(wide * wide, axis=-1, keepdims=True) + NORM_EPS)
    return (wide * inv_rms * gain.astype(jnp.float32)).astype(jnp.bfloat16)


def rope_tables(positions):
    inv_freq = jnp.asarray(ROPE_THETA, jnp.float32) ** (-jnp.arange(0, HEAD_DIM, 2, dtype=jnp.float32) / HEAD_DIM)
    angles = positions.astype(jnp.float32)[:, None] * inv_freq[None, :]
    cos, sin = jnp.cos(angles), jnp.sin(angles)
    return jnp.concatenate([cos, cos], axis=-1), jnp.concatenate([-sin, sin], axis=-1)


def rope_head(head, cos_t, sin_t):
    wide = head.astype(jnp.bfloat16).astype(jnp.float32)
    return (wide * cos_t + pltpu.roll(wide, HEAD_DIM // 2, 1) * sin_t).astype(jnp.bfloat16)


def kv_kernel(x_ref, gain_ref, cos_ref, sin_ref, w_k_ref, w_v_ref, kv_ref):
    normed = rms_norm(x_ref[...], gain_ref[...])
    width = w_k_ref.shape[1]
    keys = jnp.dot(normed, w_k_ref[...], preferred_element_type=jnp.float32)
    for head in range(width // HEAD_DIM):
        cols = slice(head * HEAD_DIM, (head + 1) * HEAD_DIM)
        kv_ref[:, cols] = rope_head(keys[:, cols], cos_ref[...], sin_ref[...])
    kv_ref[:, width:] = jnp.dot(normed, w_v_ref[...], preferred_element_type=jnp.float32).astype(jnp.bfloat16)


def q_kernel(x_ref, gain_ref, cos_ref, sin_ref, w_q_ref, q_ref):
    normed = rms_norm(x_ref[...], gain_ref[...])
    queries = jnp.dot(normed, w_q_ref[...], preferred_element_type=jnp.float32)
    for head in range(w_q_ref.shape[1] // HEAD_DIM):
        cols = slice(head * HEAD_DIM, (head + 1) * HEAD_DIM)
        q_ref[:, cols] = rope_head(queries[:, cols], cos_ref[...], sin_ref[...])


def project(kernel, x, gain, cos_tab, sin_tab, weights, out_cols):
    rows, dim = x.shape
    row_block = lambda cols: pl.BlockSpec((ROW_TILE, cols), lambda i: (i, 0))
    w_cols = sum(w.shape[1] for w in weights)
    return pl.pallas_call(
        kernel,
        out_shape=jax.ShapeDtypeStruct((rows, out_cols), jnp.bfloat16),
        grid=(rows // ROW_TILE,),
        in_specs=[row_block(dim), pl.BlockSpec((1, dim), lambda i: (0, 0)), row_block(HEAD_DIM), row_block(HEAD_DIM)]
        + [pl.BlockSpec(w.shape, lambda i: (0, 0), pipeline_mode=pl.Buffered(1)) for w in weights],
        out_specs=row_block(out_cols),
        compiler_params=pltpu.CompilerParams(vmem_limit_bytes=VMEM_LIMIT),
        cost_estimate=pl.CostEstimate(flops=2 * rows * dim * w_cols, bytes_accessed=2 * dim * (rows + w_cols), transcendentals=0),
    )(x, gain.reshape(1, dim), cos_tab, sin_tab, *weights)


def flash(queries, blocks, chunk, rows, kv_head, kv_heads, axis, cp_size, after=()):
    q_cols = queries.shape[1] // kv_heads
    heads = q_cols // HEAD_DIM
    span = blocks[0].shape[0]
    row_start = chunk * rows

    def kernel(q_ref, *rest):
        block_refs, (o_ref, k_buf, v_buf, m_ref, l_ref, acc_ref, sems) = rest[:8], rest[8 + len(after):]
        index = lax.axis_index(axis)
        odd = lax.rem(index, 2)
        slots = [0, 2, 4, 6] + [jnp.where(odd == 1, a, b) for a, b in ((1, 7), (3, 1), (5, 3), (7, 5))]
        copies = []
        for n, slot in enumerate(slots):
            start = slot * span if n < 4 else pl.multiple_of(slot * span, span)
            for part, buf in enumerate((k_buf, v_buf)):
                col = (part * kv_heads + kv_head) * HEAD_DIM
                copies.append(pltpu.make_async_copy(block_refs[n].at[:, col:col + HEAD_DIM], buf.at[pl.ds(start, span)], sems.at[2 * n + part]))
        for copy in copies:
            copy.start()

        def tile_step(start, masked):
            k_tile = k_buf[pl.ds(start, KEY_TILE)]
            v_tile = v_buf[pl.ds(start, KEY_TILE)]
            for head in range(heads):
                scores = lax.dot_general(q_ref[:, head * HEAD_DIM:(head + 1) * HEAD_DIM], k_tile, (((1,), (1,)), ((), ())), preferred_element_type=jnp.float32)
                if masked:
                    q_pos = row_start + lax.broadcasted_iota(jnp.int32, scores.shape, 0)
                    k_pos = start + lax.broadcasted_iota(jnp.int32, scores.shape, 1)
                    scores = jnp.where(k_pos <= q_pos, scores, MASK_VALUE)
                parts = [scores[:, n:n + 128] for n in range(0, KEY_TILE, 128)]
                new_max = jnp.broadcast_to(jnp.max(functools.reduce(jnp.maximum, parts), axis=1, keepdims=True), (rows, 128))
                if not masked:
                    old_max = m_ref[head]
                    new_max = jnp.maximum(old_max, new_max)
                probs = [jnp.exp2((part - new_max) * SCORE_EXP2) for part in parts]
                tile_sum = functools.reduce(jnp.add, probs)
                weighted = jnp.dot(jnp.concatenate(probs, axis=1).astype(jnp.bfloat16), v_tile, preferred_element_type=jnp.float32)
                if masked:
                    l_ref[head] = tile_sum
                    acc_ref[head] = weighted
                else:
                    rescale = jnp.exp2((old_max - new_max) * SCORE_EXP2)
                    l_ref[head] = l_ref[head] * rescale + tile_sum
                    acc_ref[head] = acc_ref[head] * rescale + weighted
                m_ref[head] = new_max

        for copy in copies[:2]:
            copy.wait()
        own_full = row_start // KEY_TILE
        tile_step(own_full * KEY_TILE, True)
        for copy in copies[2:]:
            copy.wait()
        per_block = span // KEY_TILE

        def full_step(i, carry):
            tile = jnp.where(i < own_full, i, i - own_full + per_block)
            tile_step(pl.multiple_of(tile * KEY_TILE, KEY_TILE), False)
            return carry

        lax.fori_loop(0, own_full + index * per_block, full_step, 0)
        for head in range(heads):
            total = jnp.sum(l_ref[head], axis=1, keepdims=True)
            o_ref[:, head * HEAD_DIM:(head + 1) * HEAD_DIM] = (acc_ref[head] / total).astype(jnp.bfloat16)

    return pl.pallas_call(
        kernel,
        out_shape=jax.ShapeDtypeStruct((rows, q_cols), jnp.bfloat16),
        grid=(1,),
        in_specs=[pl.BlockSpec((rows, q_cols), lambda i: (chunk, kv_head))] + [pl.BlockSpec(memory_space=pl.ANY)] * (8 + len(after)),
        out_specs=pl.BlockSpec((rows, q_cols), lambda i: (0, 0)),
        scratch_shapes=[
            pltpu.VMEM((cp_size * span, HEAD_DIM), jnp.bfloat16),
            pltpu.VMEM((cp_size * span, HEAD_DIM), jnp.bfloat16),
            pltpu.VMEM((heads, rows, 128), jnp.float32),
            pltpu.VMEM((heads, rows, 128), jnp.float32),
            pltpu.VMEM((heads, rows, HEAD_DIM), jnp.float32),
            pltpu.SemaphoreType.DMA((16,)),
        ],
        compiler_params=pltpu.CompilerParams(vmem_limit_bytes=VMEM_LIMIT),
        cost_estimate=pl.CostEstimate(flops=4 * rows * q_cols * span * cp_size, bytes_accessed=4 * cp_size * span * HEAD_DIM, transcendentals=0),
    )(queries, *blocks, *after)


def pieces_out(value, refs):
    half = refs[0].shape[0]
    for n, ref in enumerate(refs):
        ref[...] = value[n * half:(n + 1) * half].astype(jnp.bfloat16)


def out_proj(heads, w_o, axis, size, col_tile, after=()):
    rows = heads[0].shape[0]
    width = [h.shape[1] for h in heads]
    depth, dim = w_o.shape
    piece = rows // size
    half = piece // 2

    def kernel(*refs):
        head_refs, w_ref, outs, turned = refs[:len(heads)], refs[len(heads)], refs[len(heads) + 1 + len(after):-1], refs[-1]

        @pl.when(pl.program_id(0) == 0)
        def _():
            index = lax.axis_index(axis)
            for place, step in enumerate((0, size - 1, 1, 2)):
                start = pl.multiple_of(lax.rem(index + step, size) * piece, piece)
                col = 0
                for ref, cols in zip(head_refs, width):
                    turned[place * piece:(place + 1) * piece, col:col + cols] = ref[pl.ds(start, piece), :]
                    col += cols

        pieces_out(jnp.dot(turned[...], w_ref[...], preferred_element_type=jnp.float32), outs)

    return pl.pallas_call(
        kernel,
        out_shape=[jax.ShapeDtypeStruct((half, dim), jnp.bfloat16)] * (2 * size),
        grid=(dim // col_tile,),
        in_specs=[pl.BlockSpec((rows, cols), lambda i: (0, 0)) for cols in width] + [pl.BlockSpec((depth, col_tile), lambda i: (0, i))]
        + [pl.BlockSpec(memory_space=pl.ANY)] * len(after),
        out_specs=[pl.BlockSpec((half, col_tile), lambda i: (0, i))] * (2 * size),
        scratch_shapes=[pltpu.VMEM((rows, depth), jnp.bfloat16)],
        compiler_params=pltpu.CompilerParams(vmem_limit_bytes=VMEM_LIMIT),
        cost_estimate=pl.CostEstimate(flops=2 * rows * depth * dim, bytes_accessed=2 * depth * dim + 4 * rows * dim, transcendentals=0),
    )(*heads, w_o, *after)


def gate_up(pieces, w_gate, w_up, col_tile, after=()):
    half, dim = pieces[0].shape
    rows = half * len(pieces)
    width = w_gate.shape[1]

    def kernel(*refs):
        piece_refs, (w_gate_ref, w_up_ref), (out_ref, normed, sem) = refs[:len(pieces)], refs[len(pieces):len(pieces) + 2], refs[-3:]

        @pl.when(pl.program_id(0) == 0)
        def _():
            copies = [pltpu.make_async_copy(ref, normed.at[n * half:(n + 1) * half], sem.at[n]) for n, ref in enumerate(piece_refs)]
            for copy in copies:
                copy.start()
            for copy in copies:
                copy.wait()

        gate = jnp.dot(normed[...], w_gate_ref[...], preferred_element_type=jnp.float32)
        up = jnp.dot(normed[...], w_up_ref[...], preferred_element_type=jnp.float32)
        out_ref[...] = (jax.nn.silu(gate) * up).astype(jnp.bfloat16)

    return pl.pallas_call(
        kernel,
        out_shape=jax.ShapeDtypeStruct((rows, width), jnp.bfloat16),
        grid=(width // col_tile,),
        in_specs=[pl.BlockSpec(memory_space=pl.ANY)] * len(pieces) + [pl.BlockSpec((dim, col_tile), lambda i: (0, i))] * 2
        + [pl.BlockSpec(memory_space=pl.ANY)] * len(after),
        out_specs=pl.BlockSpec((rows, col_tile), lambda i: (0, i)),
        scratch_shapes=[pltpu.VMEM((rows, dim), jnp.bfloat16), pltpu.SemaphoreType.DMA((len(pieces),))],
        compiler_params=pltpu.CompilerParams(vmem_limit_bytes=VMEM_LIMIT),
        cost_estimate=pl.CostEstimate(flops=4 * rows * dim * width, bytes_accessed=4 * dim * width + 2 * rows * (dim + width), transcendentals=0),
    )(*pieces, w_gate, w_up, *after)


def down_proj(activated, w_down, n_pieces, col_tile, after=()):
    rows, depth = activated.shape
    dim = w_down.shape[1]
    half = rows // n_pieces

    def kernel(*refs):
        act_ref, w_ref, outs = refs[0], refs[1], refs[2 + len(after):]
        pieces_out(jnp.dot(act_ref[...], w_ref[...], preferred_element_type=jnp.float32), outs)

    return pl.pallas_call(
        kernel,
        out_shape=[jax.ShapeDtypeStruct((half, dim), jnp.bfloat16)] * n_pieces,
        grid=(dim // col_tile,),
        in_specs=[pl.BlockSpec((rows, depth), lambda i: (0, 0), pipeline_mode=pl.Buffered(1)), pl.BlockSpec((depth, col_tile), lambda i: (0, i))]
        + [pl.BlockSpec(memory_space=pl.ANY)] * len(after),
        out_specs=[pl.BlockSpec((half, col_tile), lambda i: (0, i))] * n_pieces,
        compiler_params=pltpu.CompilerParams(vmem_limit_bytes=VMEM_LIMIT),
        cost_estimate=pl.CostEstimate(flops=2 * rows * depth * dim, bytes_accessed=2 * depth * dim + 4 * rows * dim, transcendentals=0),
    )(activated, w_down, *after)


def assemble(chunks, axis, size):
    half, dim = chunks[0][0].shape
    per_chunk = len(chunks[0])
    flat = [piece for pieces in chunks for piece in pieces]
    total = half * len(flat)

    def kernel(*refs):
        ins, (out_ref, buf, in_sem, out_sem) = refs[:len(flat)], refs[len(flat):]
        index = lax.axis_index(axis)
        places = []
        for n in range(len(flat)):
            step = (0, size - 1, 1, 2)[n % per_chunk // 2]
            start = (n // per_chunk * per_chunk + n % 2 + 2 * lax.rem(index + step, size)) * half
            places.append(pl.ds(pl.multiple_of(start, half), half))
        loads = [pltpu.make_async_copy(ref, buf.at[n], in_sem.at[n]) for n, ref in enumerate(ins)]
        stores = [pltpu.make_async_copy(buf.at[n], out_ref.at[places[n]], out_sem.at[n]) for n in range(len(flat))]
        for load in loads:
            load.start()
        for load, store in zip(loads, stores):
            load.wait()
            store.start()
        for store in stores:
            store.wait()

    return pl.pallas_call(
        kernel,
        out_shape=jax.ShapeDtypeStruct((total, dim), jnp.bfloat16),
        in_specs=[pl.BlockSpec(memory_space=pl.ANY)] * len(flat),
        out_specs=pl.BlockSpec(memory_space=pl.ANY),
        scratch_shapes=[pltpu.VMEM((len(flat), half, dim), jnp.bfloat16), pltpu.SemaphoreType.DMA((len(flat),)), pltpu.SemaphoreType.DMA((len(flat),))],
        compiler_params=pltpu.CompilerParams(vmem_limit_bytes=VMEM_LIMIT),
        cost_estimate=pl.CostEstimate(flops=0, bytes_accessed=4 * total * dim, transcendentals=0),
    )(*flat)


def scatter_first(parts, fwd, back):
    own_lo, own_hi, prev_lo, prev_hi, next_lo, next_hi, far_lo, far_hi = parts
    return fwd(far_lo), back(far_hi), fwd(next_hi), back(prev_lo)


def scatter_second(parts, first, fwd, back):
    passed_lo, passed_hi = first[:2]
    add = lambda a, b: (a.astype(jnp.float32) + b.astype(jnp.float32)).astype(jnp.bfloat16)
    return fwd(add(parts[4], passed_lo)), back(add(parts[3], passed_hi))


def scatter_sum(base, parts, first, second):
    wide = lambda *terms: functools.reduce(jnp.add, [t.astype(jnp.float32) for t in terms]).astype(jnp.bfloat16)
    return wide(base[0], parts[0], second[0], first[3]), wide(base[1], parts[1], first[2], second[1])


def spread_first(lo, hi, fwd, back):
    return fwd(lo), back(hi), fwd(hi), back(lo)


def spread_second(first, fwd, back):
    return fwd(first[0]), back(first[1])


def spread_pieces(lo, hi, first, second):
    prev_lo, next_hi, prev_hi, next_lo = first
    return [lo, hi, prev_lo, prev_hi, next_lo, next_hi, second[0], second[1]]


def permuter(axis, pairs):
    return lambda value: lax.ppermute(value, axis, pairs)


def solution(mesh):
    cp_size = mesh.shape['cp']
    tp_size = mesh.shape['tp']
    row_spec = P(('dp', 'cp'), None)
    cache_spec = P(('dp', 'cp'), 'tp', None)
    col_spec = P(None, 'tp')
    split_rows = P('tp', None)
    vec_spec = P(None)

    def local_layer(x, attn_gain, w_q, w_k, w_v, w_o, mlp_gain, w_gate, w_up, w_down):
        tok_dev = x.shape[0]
        kv_local = w_k.shape[1] // HEAD_DIM
        kv_cols = w_k.shape[1]
        cp_index = lax.axis_index('cp')
        tp_index = lax.axis_index('tp')
        ahead = permuter('cp', [(s, (s + 2) % cp_size) for s in range(cp_size)])
        behind = permuter('cp', [(s, (s - 2) % cp_size) for s in range(cp_size)])
        swap = permuter('cp', [(s, s ^ 1) for s in range(cp_size)])
        fwd = permuter('tp', [(s, (s + 1) % tp_size) for s in range(tp_size)])
        back = permuter('tp', [(s, (s - 1) % tp_size) for s in range(tp_size)])
        cos_tab, sin_tab = rope_tables(cp_index * tok_dev + jnp.arange(tok_dev))
        own = project(kv_kernel, x, attn_gain, cos_tab, sin_tab, [w_k, w_v], 2 * kv_cols)
        middle = tok_dev // 2
        low, high, mate = ahead(own), behind(own), swap(own)
        queries = project(q_kernel, x, attn_gain, cos_tab, sin_tab, [w_q], w_q.shape[1])
        low, high, queries = lax.optimization_barrier((low, high, queries))
        far = jnp.concatenate([ahead(low[:middle]), behind(high[middle:])], axis=0)
        blocks = [own, low, far, high, mate, swap(low), swap(far), swap(high)]
        rows = tok_dev // 2
        piece = rows // tp_size
        half = piece // 2

        def attend(chunk, kv_head, after=()):
            return flash(queries, blocks, chunk, rows, kv_head, kv_local, 'cp', cp_size, after)

        def base_rows(chunk):
            start = chunk * rows + tp_index * piece
            return lax.dynamic_slice_in_dim(x, start, half, axis=0), lax.dynamic_slice_in_dim(x, start + half, half, axis=0)

        heads0 = [attend(0, n) for n in range(kv_local)]
        part0 = out_proj(heads0, w_o, 'tp', tp_size, COL_TILE)
        first0 = scatter_first(part0, fwd, back)
        heads1 = [attend(1, 0, after=part0[:1])]
        second0 = scatter_second(part0, first0, fwd, back)
        heads1.append(attend(1, 1, after=(heads1[0], first0[0], first0[1])))
        hid0 = scatter_sum(base_rows(0), part0, first0, second0)
        norm0 = [rms_norm(h, mlp_gain) for h in hid0]
        spread0 = spread_first(*norm0, fwd, back)
        part1 = out_proj(heads1, w_o, 'tp', tp_size, COL_TILE, after=(norm0[0], norm0[1]))
        first1 = scatter_first(part1, fwd, back)
        again0 = spread_second(spread0, fwd, back)
        act0 = gate_up(spread_pieces(*norm0, spread0, again0), w_gate, w_up, FF_TILE, after=(part1[0],))
        second1 = scatter_second(part1, first1, fwd, back)
        down0 = down_proj(act0, w_down, 2 * tp_size, COL_TILE, after=(first1[0], first1[1]))
        hid1 = scatter_sum(base_rows(1), part1, first1, second1)
        norm1 = [rms_norm(h, mlp_gain) for h in hid1]
        spread1 = spread_first(*norm1, fwd, back)
        again1 = spread_second(spread1, fwd, back)
        dfirst0 = scatter_first(down0, fwd, back)
        act1 = gate_up(spread_pieces(*norm1, spread1, again1), w_gate, w_up, FF_TILE, after=(down0[0],))
        dsecond0 = scatter_second(down0, dfirst0, fwd, back)
        down1 = down_proj(act1, w_down, 2 * tp_size, COL_TILE, after=(dfirst0[0], dfirst0[1]))
        out0 = scatter_sum(hid0, down0, dfirst0, dsecond0)
        gath0 = spread_first(*out0, fwd, back)
        dfirst1 = scatter_first(down1, fwd, back)
        gagain0 = spread_second(gath0, fwd, back)
        dsecond1 = scatter_second(down1, dfirst1, fwd, back)
        out1 = scatter_sum(hid1, down1, dfirst1, dsecond1)
        gath1 = spread_first(*out1, fwd, back)
        gagain1 = spread_second(gath1, fwd, back)
        x_out = assemble([spread_pieces(*out0, gath0, gagain0), spread_pieces(*out1, gath1, gagain1)], 'tp', tp_size)
        cache_shape = (tok_dev, kv_local, HEAD_DIM)
        return x_out, own[:, :kv_cols].reshape(cache_shape), own[:, kv_cols:].reshape(cache_shape)

    return jax.shard_map(local_layer, mesh=mesh,
                         in_specs=(row_spec, vec_spec, col_spec, col_spec, col_spec, split_rows, vec_spec, col_spec, col_spec, split_rows),
                         out_specs=(row_spec, cache_spec, cache_spec), check_vma=False)
```

```python
import functools
import math
import jax
import jax.numpy as jnp
from jax import lax
from jax.experimental import pallas as pl
from jax.experimental.pallas import tpu as pltpu
from jax.sharding import PartitionSpec as P

HEAD_DIM = 128
ROPE_THETA = 1000000.0
NORM_EPS = 1e-5
MASK_VALUE = -1e30
SCORE_EXP2 = HEAD_DIM ** -0.5 * math.log2(math.e)
KEY_TILE = 1024
ROW_TILE = 256
COL_TILE = 1024
FF_TILE = 512
VMEM_LIMIT = 60 * 1024 * 1024


def rms_norm(rows, gain):
    wide = rows.astype(jnp.float32)
    inv_rms = lax.rsqrt(jnp.mean(wide * wide, axis=-1, keepdims=True) + NORM_EPS)
    return (wide * inv_rms * gain.astype(jnp.float32)).astype(jnp.bfloat16)


def rope_tables(positions):
    inv_freq = jnp.asarray(ROPE_THETA, jnp.float32) ** (-jnp.arange(0, HEAD_DIM, 2, dtype=jnp.float32) / HEAD_DIM)
    angles = positions.astype(jnp.float32)[:, None] * inv_freq[None, :]
    cos, sin = jnp.cos(angles), jnp.sin(angles)
    return jnp.concatenate([cos, cos], axis=-1), jnp.concatenate([-sin, sin], axis=-1)


def rope_head(head, cos_t, sin_t):
    wide = head.astype(jnp.bfloat16).astype(jnp.float32)
    return (wide * cos_t + pltpu.roll(wide, HEAD_DIM // 2, 1) * sin_t).astype(jnp.bfloat16)


def kv_kernel(x_ref, gain_ref, cos_ref, sin_ref, w_k_ref, w_v_ref, kv_ref):
    normed = rms_norm(x_ref[...], gain_ref[...])
    width = w_k_ref.shape[1]
    keys = jnp.dot(normed, w_k_ref[...], preferred_element_type=jnp.float32)
    for head in range(width // HEAD_DIM):
        cols = slice(head * HEAD_DIM, (head + 1) * HEAD_DIM)
        kv_ref[:, cols] = rope_head(keys[:, cols], cos_ref[...], sin_ref[...])
    kv_ref[:, width:] = jnp.dot(normed, w_v_ref[...], preferred_element_type=jnp.float32).astype(jnp.bfloat16)


def q_kernel(x_ref, gain_ref, cos_ref, sin_ref, w_q_ref, q_ref):
    normed = rms_norm(x_ref[...], gain_ref[...])
    queries = jnp.dot(normed, w_q_ref[...], preferred_element_type=jnp.float32)
    for head in range(w_q_ref.shape[1] // HEAD_DIM):
        cols = slice(head * HEAD_DIM, (head + 1) * HEAD_DIM)
        q_ref[:, cols] = rope_head(queries[:, cols], cos_ref[...], sin_ref[...])


def project(kernel, x, gain, cos_tab, sin_tab, weights, out_cols):
    rows, dim = x.shape
    row_block = lambda cols: pl.BlockSpec((ROW_TILE, cols), lambda i: (i, 0))
    w_cols = sum(w.shape[1] for w in weights)
    return pl.pallas_call(
        kernel,
        out_shape=jax.ShapeDtypeStruct((rows, out_cols), jnp.bfloat16),
        grid=(rows // ROW_TILE,),
        in_specs=[row_block(dim), pl.BlockSpec((1, dim), lambda i: (0, 0)), row_block(HEAD_DIM), row_block(HEAD_DIM)]
        + [pl.BlockSpec(w.shape, lambda i: (0, 0), pipeline_mode=pl.Buffered(1)) for w in weights],
        out_specs=row_block(out_cols),
        compiler_params=pltpu.CompilerParams(vmem_limit_bytes=VMEM_LIMIT),
        cost_estimate=pl.CostEstimate(flops=2 * rows * dim * w_cols, bytes_accessed=2 * dim * (rows + w_cols), transcendentals=0),
    )(x, gain.reshape(1, dim), cos_tab, sin_tab, *weights)


class Ring:
    n_remote = 12

    def __init__(self, axis, size, partial, base, base_row, gain, ring_id):
        self.axis, self.size, self.base_row, self.ring_id = axis, size, base_row, ring_id
        self.pieces, self.half, self.dim = partial.shape
        self.normed = gain is not None
        self.operands = [partial, base] + ([gain.reshape(1, self.dim)] if self.normed else [])
        any_spec = pl.BlockSpec(memory_space=pl.ANY)
        self.in_specs = [any_spec, any_spec] + ([pl.BlockSpec(memory_space=pltpu.VMEM)] if self.normed else [])
        shapes = [(self.pieces, self.half, self.dim)] + ([(2, self.half, self.dim)] if self.normed else [])
        self.out_shape = [jax.ShapeDtypeStruct(shape, jnp.bfloat16) for shape in shapes]
        self.out_specs = [any_spec] * len(shapes)
        buf = lambda n: pltpu.VMEM((n, self.half, self.dim), jnp.bfloat16)
        self.scratch = [buf(6), buf(6), buf(2), pltpu.SemaphoreType.DMA((self.n_remote,)), pltpu.SemaphoreType.DMA((self.n_remote,)), pltpu.SemaphoreType.DMA((10,))]

    def bind(self, ins, outs, scratch):
        partial, base = ins[:2]
        gathered = outs[0]
        arrived, local, sent, self.send_sem, self.recv_sem, self.local_sem = scratch
        index = lax.axis_index(self.axis)
        fwd, back = lax.rem(index + 1, self.size), lax.rem(index + self.size - 1, self.size)
        self.neighbours = (fwd, back)
        self.arrived, self.local, self.sent = arrived, local, sent
        self.gain = ins[2] if self.normed else None
        self.remote = [
            (partial.at[6], arrived.at[0], fwd), (partial.at[7], arrived.at[1], back),
            (partial.at[5], arrived.at[2], fwd), (partial.at[2], arrived.at[3], back),
            (local.at[0], arrived.at[4], fwd), (local.at[1], arrived.at[5], back),
            (sent.at[0], gathered.at[2], fwd), (sent.at[1], gathered.at[5], back),
            (sent.at[1], gathered.at[3], fwd), (sent.at[0], gathered.at[4], back),
            (gathered.at[2], gathered.at[6], fwd), (gathered.at[5], gathered.at[7], back),
        ]
        if self.base_row is None:
            rows = [base.at[0], base.at[1]]
        else:
            start = pl.multiple_of(self.base_row + index * (2 * self.half), self.half)
            rows = [base.at[pl.ds(start, self.half)], base.at[pl.ds(pl.multiple_of(start + self.half, self.half), self.half)]]
        self.copies = [
            (partial.at[4], local.at[0]), (partial.at[3], local.at[1]), (partial.at[0], local.at[2]), (partial.at[1], local.at[3]),
            (rows[0], local.at[4]), (rows[1], local.at[5]), (sent.at[0], gathered.at[0]), (sent.at[1], gathered.at[1]),
        ] + ([(local.at[4], outs[1].at[0]), (local.at[5], outs[1].at[1])] if self.normed else [])

    def rdma(self, n):
        src, dst, peer = self.remote[n]
        return pltpu.make_async_remote_copy(src_ref=src, dst_ref=dst, send_sem=self.send_sem.at[n], recv_sem=self.recv_sem.at[n],
                                            device_id={self.axis: peer}, device_id_type=pl.DeviceIdType.MESH)

    def copy(self, n):
        src, dst = self.copies[n]
        return pltpu.make_async_copy(src, dst, self.local_sem.at[n])

    def step(self, n):
        (self.begin, self.pass_on, self.add_up, self.relay, self.finish)[n]()

    def begin(self):
        barrier = pltpu.get_barrier_semaphore()
        for peer in self.neighbours:
            pl.semaphore_signal(barrier, inc=1, device_id={self.axis: peer}, device_id_type=pl.DeviceIdType.MESH)
        for n in range(6):
            self.copy(n).start()
        pl.semaphore_wait(barrier, 2)
        for n in range(4):
            self.rdma(n).start()

    def pass_on(self):
        for n in range(2):
            self.copy(n).wait()
            self.rdma(n).wait_recv()
            self.local[n] = (self.local[n].astype(jnp.float32) + self.arrived[n].astype(jnp.float32)).astype(jnp.bfloat16)
        for n in range(2):
            self.rdma(4 + n).start()

    def add_up(self):
        for n in range(2, 6):
            self.copy(n).wait()
            self.rdma(n).wait_recv()
        for n, (a, b) in enumerate(((4, 3), (2, 5))):
            terms = (self.local[4 + n], self.local[2 + n], self.arrived[a], self.arrived[b])
            total = functools.reduce(jnp.add, [term.astype(jnp.float32) for term in terms]).astype(jnp.bfloat16)
            if self.normed:
                self.local[4 + n] = total
                self.sent[n] = rms_norm(total, self.gain[...])
            else:
                self.sent[n] = total
        for n in range(6, 10):
            self.rdma(n).start()
        for n in range(6, len(self.copies)):
            self.copy(n).start()

    def relay(self):
        for n in range(2):
            self.rdma(6 + n).wait_recv()
            self.rdma(10 + n).start()

    def finish(self):
        for n in range(8, 12):
            self.rdma(n).wait_recv()
        for n in range(12):
            self.rdma(n).wait_send()
        for n in range(6, len(self.copies)):
            self.copy(n).wait()


def params(ring):
    if ring is None:
        return pltpu.CompilerParams(vmem_limit_bytes=VMEM_LIMIT)
    return pltpu.CompilerParams(vmem_limit_bytes=VMEM_LIMIT, collective_id=ring.ring_id, has_side_effects=True)


def host(kernel, ring, operands, in_specs, out_shape, out_specs, scratch, grid, flops, nbytes):
    n_in, n_ring = len(operands), len(ring.operands) if ring else 0

    def body(*refs):
        ins, rest = refs[:n_in], refs[n_in:]
        ring_ins, rest = rest[:n_ring], rest[n_ring:]
        out, rest = rest[0], rest[1:]
        if ring:
            ring_outs, rest = rest[:len(ring.out_shape)], rest[len(ring.out_shape):]
            ring.bind(ring_ins, ring_outs, rest[len(scratch):])
        kernel(ins, out, rest[:len(scratch)], ring)

    out = pl.pallas_call(
        body,
        out_shape=[out_shape] + (ring.out_shape if ring else []),
        grid=grid,
        in_specs=in_specs + (ring.in_specs if ring else []),
        out_specs=[out_specs] + (ring.out_specs if ring else []),
        scratch_shapes=scratch + (ring.scratch if ring else []),
        compiler_params=params(ring),
        cost_estimate=pl.CostEstimate(flops=flops, bytes_accessed=nbytes, transcendentals=0),
    )(*operands, *(ring.operands if ring else []))
    return out if ring else out[0]


def flash(queries, blocks, chunk, rows, kv_heads, axis, cp_size, ring=None):
    q_cols = queries.shape[1] // kv_heads
    heads = q_cols // HEAD_DIM
    span = blocks[0].shape[0]
    row_start = chunk * rows

    def kernel(ins, o_ref, scratch, ring):
        q_ref, block_refs = ins[0], ins[1:]
        k_buf, v_buf, m_ref, l_ref, acc_ref, sems = scratch
        kv_head = pl.program_id(0)
        index = lax.axis_index(axis)
        odd = lax.rem(index, 2)
        if ring:
            pl.when(kv_head == 0)(ring.begin)
        slots = [0, 2, 4, 6] + [jnp.where(odd == 1, a, b) for a, b in ((1, 7), (3, 1), (5, 3), (7, 5))]
        copies = []
        for n, slot in enumerate(slots):
            start = slot * span if n < 4 else pl.multiple_of(slot * span, span)
            for part, buf in enumerate((k_buf, v_buf)):
                col = pl.multiple_of((part * kv_heads + kv_head) * HEAD_DIM, HEAD_DIM)
                copies.append(pltpu.make_async_copy(block_refs[n].at[:, pl.ds(col, HEAD_DIM)], buf.at[pl.ds(start, span)], sems.at[2 * n + part]))
        for copy in copies:
            copy.start()

        def tile_step(start, masked):
            k_tile = k_buf[pl.ds(start, KEY_TILE)]
            v_tile = v_buf[pl.ds(start, KEY_TILE)]
            for head in range(heads):
                scores = lax.dot_general(q_ref[:, head * HEAD_DIM:(head + 1) * HEAD_DIM], k_tile, (((1,), (1,)), ((), ())), preferred_element_type=jnp.float32)
                if masked:
                    q_pos = row_start + lax.broadcasted_iota(jnp.int32, scores.shape, 0)
                    k_pos = start + lax.broadcasted_iota(jnp.int32, scores.shape, 1)
                    scores = jnp.where(k_pos <= q_pos, scores, MASK_VALUE)
                parts = [scores[:, n:n + 128] for n in range(0, KEY_TILE, 128)]
                new_max = jnp.broadcast_to(jnp.max(functools.reduce(jnp.maximum, parts), axis=1, keepdims=True), (rows, 128))
                if not masked:
                    old_max = m_ref[head]
                    new_max = jnp.maximum(old_max, new_max)
                probs = [jnp.exp2((part - new_max) * SCORE_EXP2) for part in parts]
                tile_sum = functools.reduce(jnp.add, probs)
                weighted = jnp.dot(jnp.concatenate(probs, axis=1).astype(jnp.bfloat16), v_tile, preferred_element_type=jnp.float32)
                if masked:
                    l_ref[head] = tile_sum
                    acc_ref[head] = weighted
                else:
                    rescale = jnp.exp2((old_max - new_max) * SCORE_EXP2)
                    l_ref[head] = l_ref[head] * rescale + tile_sum
                    acc_ref[head] = acc_ref[head] * rescale + weighted
                m_ref[head] = new_max

        for copy in copies[:2]:
            copy.wait()
        own_full = row_start // KEY_TILE
        tile_step(own_full * KEY_TILE, True)
        for copy in copies[2:]:
            copy.wait()
        per_block = span // KEY_TILE
        n_full = own_full + index * per_block
        trips = jnp.maximum(n_full, 4) if ring else n_full

        def full_step(i, carry):
            if ring:
                pl.when((kv_head == 0) & (i == trips * 3 // 5))(ring.pass_on)
                pl.when((kv_head == 1) & (i == trips // 4))(ring.add_up)
                pl.when((kv_head == 1) & (i == trips * 3 // 4))(ring.relay)

            @pl.when(i < n_full)
            def _():
                tile = jnp.where(i < own_full, i, i - own_full + per_block)
                tile_step(pl.multiple_of(tile * KEY_TILE, KEY_TILE), False)
            return carry

        lax.fori_loop(0, trips, full_step, 0)
        for head in range(heads):
            total = jnp.sum(l_ref[head], axis=1, keepdims=True)
            o_ref[:, head * HEAD_DIM:(head + 1) * HEAD_DIM] = (acc_ref[head] / total).astype(jnp.bfloat16)
        if ring:
            pl.when(kv_head == 1)(ring.finish)

    return host(
        kernel, ring, [queries] + blocks,
        [pl.BlockSpec((rows, q_cols), lambda i: (chunk, i))] + [pl.BlockSpec(memory_space=pl.ANY)] * 8,
        jax.ShapeDtypeStruct((rows, q_cols * kv_heads), jnp.bfloat16), pl.BlockSpec((rows, q_cols), lambda i: (0, i)),
        [
            pltpu.VMEM((cp_size * span, HEAD_DIM), jnp.bfloat16),
            pltpu.VMEM((cp_size * span, HEAD_DIM), jnp.bfloat16),
            pltpu.VMEM((heads, rows, 128), jnp.float32),
            pltpu.VMEM((heads, rows, 128), jnp.float32),
            pltpu.VMEM((heads, rows, HEAD_DIM), jnp.float32),
            pltpu.SemaphoreType.DMA((16,)),
        ],
        (kv_heads,), 4 * rows * q_cols * kv_heads * span * cp_size, 4 * kv_heads * cp_size * span * HEAD_DIM)


def out_proj(heads, w_o, axis, size, col_tile):
    rows, depth = heads.shape
    dim = w_o.shape[1]
    piece = rows // size
    half = piece // 2

    def kernel(ins, out_ref, scratch, ring):
        (head_ref, w_ref), (turned,) = ins, scratch

        @pl.when(pl.program_id(0) == 0)
        def _():
            index = lax.axis_index(axis)
            for place, step in enumerate((0, size - 1, 1, 2)):
                start = pl.multiple_of(lax.rem(index + step, size) * piece, piece)
                turned[place * piece:(place + 1) * piece] = head_ref[pl.ds(start, piece), :]

        store_pieces(jnp.dot(turned[...], w_ref[...], preferred_element_type=jnp.float32), out_ref)

    return host(
        kernel, None, [heads, w_o], [pl.BlockSpec((rows, depth), lambda i: (0, 0)), pl.BlockSpec((depth, col_tile), lambda i: (0, i))],
        jax.ShapeDtypeStruct((2 * size, half, dim), jnp.bfloat16), pl.BlockSpec((2 * size, half, col_tile), lambda i: (0, 0, i)),
        [pltpu.VMEM((rows, depth), jnp.bfloat16)], (dim // col_tile,), 2 * rows * depth * dim, 2 * depth * dim + 4 * rows * dim)


def store_pieces(value, ref):
    pieces, half, unused = ref.shape
    for n in range(pieces):
        ref[n] = value[n * half:(n + 1) * half].astype(jnp.bfloat16)


def mlp(pieces, w_gate, w_up, w_down, tile, ring):
    n_pieces, half, dim = pieces.shape
    rows = n_pieces * half
    width = w_gate.shape[1]
    n_up, n_down = width // tile, dim // tile

    def kernel(ins, out_ref, scratch, ring):
        (normed_ref, gate_ref, up_ref, down_ref), (act,) = ins, scratch
        g = pl.program_id(0)
        for n, at in enumerate((0, 3, 6, 9)):
            pl.when(g == at)(functools.partial(ring.step, n))

        @pl.when(g < n_up)
        def _():
            gate = jnp.dot(normed_ref[...], gate_ref[...], preferred_element_type=jnp.float32)
            up = jnp.dot(normed_ref[...], up_ref[...], preferred_element_type=jnp.float32)
            act[:, pl.ds(pl.multiple_of(g * tile, tile), tile)] = (jax.nn.silu(gate) * up).astype(jnp.bfloat16)

        @pl.when(g >= n_up)
        def _():
            store_pieces(jnp.dot(act[...], down_ref[...], preferred_element_type=jnp.float32), out_ref)

        pl.when(g == n_up + n_down - 1)(ring.finish)

    up_spec = pl.BlockSpec((dim, tile), lambda i: (0, jnp.minimum(i, n_up - 1)))
    return host(
        kernel, ring, [pieces.reshape(rows, dim), w_gate, w_up, w_down],
        [pl.BlockSpec((rows, dim), lambda i: (0, 0), pipeline_mode=pl.Buffered(1)), up_spec, up_spec,
         pl.BlockSpec((width, tile), lambda i: (0, jnp.maximum(i - n_up, 0)))],
        jax.ShapeDtypeStruct((n_pieces, half, dim), jnp.bfloat16), pl.BlockSpec((n_pieces, half, tile), lambda i: (0, 0, jnp.maximum(i - n_up, 0))),
        [pltpu.VMEM((rows, width), jnp.bfloat16)], (n_up + n_down,), 6 * rows * dim * width, 6 * dim * width + 6 * rows * dim)


def all_reduce(ring):
    def body(*refs):
        n_in, n_out = len(ring.operands), len(ring.out_shape)
        ring.bind(refs[:n_in], refs[n_in:n_in + n_out], refs[n_in + n_out:])
        for n in range(5):
            ring.step(n)

    return pl.pallas_call(body, out_shape=ring.out_shape, in_specs=ring.in_specs, out_specs=ring.out_specs, scratch_shapes=ring.scratch,
                          compiler_params=params(ring))(*ring.operands)


def assemble(chunks, axis, size):
    n_pieces, half, dim = chunks[0].shape
    total = len(chunks) * n_pieces

    def kernel(*refs):
        ins, (out_ref, buf, in_sem, out_sem) = refs[:len(chunks)], refs[len(chunks):]
        index = lax.axis_index(axis)
        places = []
        for n in range(total):
            step = (0, size - 1, 1, 2)[n % n_pieces // 2]
            start = (n // n_pieces * n_pieces + n % 2 + 2 * lax.rem(index + step, size)) * half
            places.append(pl.ds(pl.multiple_of(start, half), half))
        loads = [pltpu.make_async_copy(ins[n // n_pieces].at[n % n_pieces], buf.at[n], in_sem.at[n]) for n in range(total)]
        stores = [pltpu.make_async_copy(buf.at[n], out_ref.at[places[n]], out_sem.at[n]) for n in range(total)]
        for load in loads:
            load.start()
        for load, store in zip(loads, stores):
            load.wait()
            store.start()
        for store in stores:
            store.wait()

    return pl.pallas_call(
        kernel,
        out_shape=jax.ShapeDtypeStruct((total * half, dim), jnp.bfloat16),
        in_specs=[pl.BlockSpec(memory_space=pl.ANY)] * len(chunks),
        out_specs=pl.BlockSpec(memory_space=pl.ANY),
        scratch_shapes=[pltpu.VMEM((total, half, dim), jnp.bfloat16), pltpu.SemaphoreType.DMA((total,)), pltpu.SemaphoreType.DMA((total,))],
        compiler_params=pltpu.CompilerParams(vmem_limit_bytes=VMEM_LIMIT),
        cost_estimate=pl.CostEstimate(flops=0, bytes_accessed=4 * total * half * dim, transcendentals=0),
    )(*chunks)


def permuter(axis, pairs):
    return lambda value: lax.ppermute(value, axis, pairs)


def solution(mesh):
    cp_size = mesh.shape['cp']
    tp_size = mesh.shape['tp']
    row_spec = P(('dp', 'cp'), None)
    cache_spec = P(('dp', 'cp'), 'tp', None)
    col_spec = P(None, 'tp')
    split_rows = P('tp', None)
    vec_spec = P(None)

    def local_layer(x, attn_gain, w_q, w_k, w_v, w_o, mlp_gain, w_gate, w_up, w_down):
        tok_dev = x.shape[0]
        kv_local = w_k.shape[1] // HEAD_DIM
        kv_cols = w_k.shape[1]
        cp_index = lax.axis_index('cp')
        ahead = permuter('cp', [(s, (s + 2) % cp_size) for s in range(cp_size)])
        behind = permuter('cp', [(s, (s - 2) % cp_size) for s in range(cp_size)])
        swap = permuter('cp', [(s, s ^ 1) for s in range(cp_size)])
        cos_tab, sin_tab = rope_tables(cp_index * tok_dev + jnp.arange(tok_dev))
        own = project(kv_kernel, x, attn_gain, cos_tab, sin_tab, [w_k, w_v], 2 * kv_cols)
        middle = tok_dev // 2
        low, high, mate = ahead(own), behind(own), swap(own)
        queries = project(q_kernel, x, attn_gain, cos_tab, sin_tab, [w_q], w_q.shape[1])
        low, high, queries = lax.optimization_barrier((low, high, queries))
        far = jnp.concatenate([ahead(low[:middle]), behind(high[middle:])], axis=0)
        blocks = [own, low, far, high, mate, swap(low), swap(far), swap(high)]
        rows = tok_dev // 2

        def attend(chunk, ring=None):
            return flash(queries, blocks, chunk, rows, kv_local, 'cp', cp_size, ring)

        def reduce_over_tp(partial, base, base_row, gain, ring_id):
            return Ring('tp', tp_size, partial, base, base_row, gain, ring_id)

        part0 = out_proj(attend(0), w_o, 'tp', tp_size, COL_TILE)
        heads1, normed0, hidden0 = attend(1, reduce_over_tp(part0, x, 0, mlp_gain, 0))
        part1 = out_proj(heads1, w_o, 'tp', tp_size, COL_TILE)
        down0, normed1, hidden1 = mlp(normed0, w_gate, w_up, w_down, FF_TILE, reduce_over_tp(part1, x, rows, mlp_gain, 1))
        down1, out0 = mlp(normed1, w_gate, w_up, w_down, FF_TILE, reduce_over_tp(down0, hidden0, None, None, 2))
        out1 = all_reduce(reduce_over_tp(down1, hidden1, None, None, 3))[0]
        x_out = assemble([out0, out1], 'tp', tp_size)
        cache_shape = (tok_dev, kv_local, HEAD_DIM)
        return x_out, own[:, :kv_cols].reshape(cache_shape), own[:, kv_cols:].reshape(cache_shape)

    return jax.shard_map(local_layer, mesh=mesh,
                         in_specs=(row_spec, vec_spec, col_spec, col_spec, col_spec, split_rows, vec_spec, col_spec, col_spec, split_rows),
                         out_specs=(row_spec, cache_spec, cache_spec), check_vma=False)
```

```python
import functools
import math
import jax
import jax.numpy as jnp
from jax import lax
from jax.experimental import pallas as pl
from jax.experimental.pallas import tpu as pltpu
from jax.sharding import PartitionSpec as P

HEAD_DIM = 128
ROPE_THETA = 1000000.0
NORM_EPS = 1e-5
MASK_VALUE = -1e30
SCORE_EXP2 = HEAD_DIM ** -0.5 * math.log2(math.e)
KEY_TILE = 1024
ROW_TILE = 256
COL_TILE = 1024
FF_TILE = 512
VMEM_LIMIT = 60 * 1024 * 1024


def rms_norm(rows, gain):
    wide = rows.astype(jnp.float32)
    inv_rms = lax.rsqrt(jnp.mean(wide * wide, axis=-1, keepdims=True) + NORM_EPS)
    return (wide * inv_rms * gain.astype(jnp.float32)).astype(jnp.bfloat16)


def rope_tables(positions):
    inv_freq = jnp.asarray(ROPE_THETA, jnp.float32) ** (-jnp.arange(0, HEAD_DIM, 2, dtype=jnp.float32) / HEAD_DIM)
    angles = positions.astype(jnp.float32)[:, None] * inv_freq[None, :]
    cos, sin = jnp.cos(angles), jnp.sin(angles)
    return jnp.concatenate([cos, cos], axis=-1), jnp.concatenate([-sin, sin], axis=-1)


def rope_head(head, cos_t, sin_t):
    wide = head.astype(jnp.bfloat16).astype(jnp.float32)
    return (wide * cos_t + pltpu.roll(wide, HEAD_DIM // 2, 1) * sin_t).astype(jnp.bfloat16)


def kv_kernel(x_ref, gain_ref, cos_ref, sin_ref, w_k_ref, w_v_ref, kv_ref):
    normed = rms_norm(x_ref[...], gain_ref[...])
    width = w_k_ref.shape[1]
    keys = jnp.dot(normed, w_k_ref[...], preferred_element_type=jnp.float32)
    for head in range(width // HEAD_DIM):
        cols = slice(head * HEAD_DIM, (head + 1) * HEAD_DIM)
        kv_ref[:, cols] = rope_head(keys[:, cols], cos_ref[...], sin_ref[...])
    kv_ref[:, width:] = jnp.dot(normed, w_v_ref[...], preferred_element_type=jnp.float32).astype(jnp.bfloat16)


def q_kernel(x_ref, gain_ref, cos_ref, sin_ref, w_q_ref, q_ref):
    normed = rms_norm(x_ref[...], gain_ref[...])
    queries = jnp.dot(normed, w_q_ref[...], preferred_element_type=jnp.float32)
    for head in range(w_q_ref.shape[1] // HEAD_DIM):
        cols = slice(head * HEAD_DIM, (head + 1) * HEAD_DIM)
        q_ref[:, cols] = rope_head(queries[:, cols], cos_ref[...], sin_ref[...])


def project(kernel, x, gain, cos_tab, sin_tab, weights, out_cols):
    rows, dim = x.shape
    row_block = lambda cols: pl.BlockSpec((ROW_TILE, cols), lambda i: (i, 0))
    w_cols = sum(w.shape[1] for w in weights)
    return pl.pallas_call(
        kernel,
        out_shape=jax.ShapeDtypeStruct((rows, out_cols), jnp.bfloat16),
        grid=(rows // ROW_TILE,),
        in_specs=[row_block(dim), pl.BlockSpec((1, dim), lambda i: (0, 0)), row_block(HEAD_DIM), row_block(HEAD_DIM)]
        + [pl.BlockSpec(w.shape, lambda i: (0, 0), pipeline_mode=pl.Buffered(1)) for w in weights],
        out_specs=row_block(out_cols),
        compiler_params=pltpu.CompilerParams(vmem_limit_bytes=VMEM_LIMIT),
        cost_estimate=pl.CostEstimate(flops=2 * rows * dim * w_cols, bytes_accessed=2 * dim * (rows + w_cols), transcendentals=0),
    )(x, gain.reshape(1, dim), cos_tab, sin_tab, *weights)


class Ring:
    n_remote, n_sub = 12, 2

    def __init__(self, axis, size, partial, base, base_row, gain, ring_id):
        self.axis, self.size, self.base_row, self.ring_id = axis, size, base_row, ring_id
        self.pieces, self.half, self.dim = partial.shape
        self.rows = self.half // self.n_sub
        self.normed = gain is not None
        self.operands = [partial, base] + ([gain.reshape(1, self.dim)] if self.normed else [])
        any_spec = pl.BlockSpec(memory_space=pl.ANY)
        self.in_specs = [any_spec, any_spec] + ([pl.BlockSpec(memory_space=pltpu.VMEM)] if self.normed else [])
        shapes = [(self.pieces, self.half, self.dim)] + ([(2, self.half, self.dim)] if self.normed else [])
        self.out_shape = [jax.ShapeDtypeStruct(shape, jnp.bfloat16) for shape in shapes]
        self.out_specs = [any_spec] * len(shapes)
        buf = lambda n: pltpu.VMEM((n, self.half, self.dim), jnp.bfloat16)
        sems = lambda n: pltpu.SemaphoreType.DMA((self.n_sub * n,))
        self.scratch = [buf(6), buf(6), buf(2), sems(self.n_remote), sems(self.n_remote), sems(10)]
        self.steps = [self.begin]
        for kind in (self.pass_on, self.add_up, self.relay):
            self.steps += [functools.partial(kind, sub) for sub in range(self.n_sub)]
        self.steps.append(self.finish)

    def bind(self, ins, outs, scratch):
        partial, base = ins[:2]
        gathered = outs[0]
        arrived, local, sent, self.send_sem, self.recv_sem, self.local_sem = scratch
        index = lax.axis_index(self.axis)
        fwd, back = lax.rem(index + 1, self.size), lax.rem(index + self.size - 1, self.size)
        self.neighbours = (fwd, back)
        self.arrived, self.local, self.sent = arrived, local, sent
        self.gain = ins[2] if self.normed else None
        self.remote, self.copies = [], []
        for sub in range(self.n_sub):
            part = pl.ds(sub * self.rows, self.rows)
            at = lambda ref, n: ref.at[n, part]
            self.remote.append([
                (at(partial, 6), at(arrived, 0), fwd), (at(partial, 7), at(arrived, 1), back),
                (at(partial, 5), at(arrived, 2), fwd), (at(partial, 2), at(arrived, 3), back),
                (at(local, 0), at(arrived, 4), fwd), (at(local, 1), at(arrived, 5), back),
                (at(sent, 0), at(gathered, 2), fwd), (at(sent, 1), at(gathered, 5), back),
                (at(sent, 1), at(gathered, 3), fwd), (at(sent, 0), at(gathered, 4), back),
                (at(gathered, 2), at(gathered, 6), fwd), (at(gathered, 5), at(gathered, 7), back),
            ])
            if self.base_row is None:
                rows = [at(base, 0), at(base, 1)]
            else:
                start = self.base_row + sub * self.rows + index * (2 * self.half)
                rows = [base.at[pl.ds(pl.multiple_of(start + n * self.half, self.rows), self.rows)] for n in range(2)]
            self.copies.append([
                (at(partial, 4), at(local, 0)), (at(partial, 3), at(local, 1)), (at(partial, 0), at(local, 2)), (at(partial, 1), at(local, 3)),
                (rows[0], at(local, 4)), (rows[1], at(local, 5)), (at(sent, 0), at(gathered, 0)), (at(sent, 1), at(gathered, 1)),
            ] + ([(at(local, 4), at(outs[1], 0)), (at(local, 5), at(outs[1], 1))] if self.normed else []))

    def rdma(self, sub, n):
        src, dst, peer = self.remote[sub][n]
        sem = sub * self.n_remote + n
        return pltpu.make_async_remote_copy(src_ref=src, dst_ref=dst, send_sem=self.send_sem.at[sem], recv_sem=self.recv_sem.at[sem],
                                            device_id={self.axis: peer}, device_id_type=pl.DeviceIdType.MESH)

    def copy(self, sub, n):
        src, dst = self.copies[sub][n]
        return pltpu.make_async_copy(src, dst, self.local_sem.at[sub * 10 + n])

    def begin(self):
        barrier = pltpu.get_barrier_semaphore()
        for peer in self.neighbours:
            pl.semaphore_signal(barrier, inc=1, device_id={self.axis: peer}, device_id_type=pl.DeviceIdType.MESH)
        pl.semaphore_wait(barrier, 2)
        for sub in range(self.n_sub):
            for n in range(4):
                self.rdma(sub, n).start()
        for sub in range(self.n_sub):
            for n in range(6):
                self.copy(sub, n).start()

    def pass_on(self, sub):
        part = pl.ds(sub * self.rows, self.rows)
        for n in range(2):
            self.copy(sub, n).wait()
            self.rdma(sub, n).wait_recv()
            self.local[n, part] = (self.local[n, part].astype(jnp.float32) + self.arrived[n, part].astype(jnp.float32)).astype(jnp.bfloat16)
        for n in range(2):
            self.rdma(sub, 4 + n).start()

    def add_up(self, sub):
        part = pl.ds(sub * self.rows, self.rows)
        for n in range(2, 6):
            self.copy(sub, n).wait()
            self.rdma(sub, n).wait_recv()
        for n, (a, b) in enumerate(((4, 3), (2, 5))):
            terms = (self.local[4 + n, part], self.local[2 + n, part], self.arrived[a, part], self.arrived[b, part])
            total = functools.reduce(jnp.add, [term.astype(jnp.float32) for term in terms]).astype(jnp.bfloat16)
            if self.normed:
                self.local[4 + n, part] = total
                self.sent[n, part] = rms_norm(total, self.gain[...])
            else:
                self.sent[n, part] = total
        for n in range(6, 10):
            self.rdma(sub, n).start()
        for n in range(6, len(self.copies[sub])):
            self.copy(sub, n).start()

    def relay(self, sub):
        for n in range(2):
            self.rdma(sub, 6 + n).wait_recv()
            self.rdma(sub, 10 + n).start()

    def finish(self):
        for sub in range(self.n_sub):
            for n in range(8, 12):
                self.rdma(sub, n).wait_recv()
            for n in range(12):
                self.rdma(sub, n).wait_send()
            for n in range(6, len(self.copies[sub])):
                self.copy(sub, n).wait()


def params(ring):
    if ring is None:
        return pltpu.CompilerParams(vmem_limit_bytes=VMEM_LIMIT)
    return pltpu.CompilerParams(vmem_limit_bytes=VMEM_LIMIT, collective_id=ring.ring_id, has_side_effects=True)


def host(kernel, ring, operands, in_specs, out_shape, out_specs, scratch, grid, flops, nbytes):
    n_in, n_ring = len(operands), len(ring.operands) if ring else 0

    def body(*refs):
        ins, rest = refs[:n_in], refs[n_in:]
        ring_ins, rest = rest[:n_ring], rest[n_ring:]
        out, rest = rest[0], rest[1:]
        if ring:
            ring_outs, rest = rest[:len(ring.out_shape)], rest[len(ring.out_shape):]
            ring.bind(ring_ins, ring_outs, rest[len(scratch):])
        kernel(ins, out, rest[:len(scratch)], ring)

    out = pl.pallas_call(
        body,
        out_shape=[out_shape] + (ring.out_shape if ring else []),
        grid=grid,
        in_specs=in_specs + (ring.in_specs if ring else []),
        out_specs=[out_specs] + (ring.out_specs if ring else []),
        scratch_shapes=scratch + (ring.scratch if ring else []),
        compiler_params=params(ring),
        cost_estimate=pl.CostEstimate(flops=flops, bytes_accessed=nbytes, transcendentals=0),
    )(*operands, *(ring.operands if ring else []))
    return out if ring else out[0]


def attention(queries, blocks, w_o, chunk, rows, kv_heads, axis, cp_size, tp_axis, tp_size, ring=None):
    q_cols = queries.shape[1] // kv_heads
    heads = q_cols // HEAD_DIM
    span = blocks[0].shape[0]
    row_start = chunk * rows
    depth, dim = w_o.shape
    piece = rows // tp_size
    half = piece // 2
    n_cols = dim // FF_TILE

    def kernel(ins, part_ref, scratch, ring):
        q_ref, block_refs, w_ref = ins[0], ins[1:-1], ins[-1]
        k_buf, v_buf, m_ref, l_ref, acc_ref, sems, turned, w_buf, part_buf, w_sem, part_sem = scratch
        kv_head = pl.program_id(0)
        index = lax.axis_index(axis)
        odd = lax.rem(index, 2)
        if ring:
            pl.when(kv_head == 0)(ring.begin)
        slots = [0, 2, 4, 6] + [jnp.where(odd == 1, a, b) for a, b in ((1, 7), (3, 1), (5, 3), (7, 5))]
        copies = []
        for n, slot in enumerate(slots):
            start = slot * span if n < 4 else pl.multiple_of(slot * span, span)
            for part, buf in enumerate((k_buf, v_buf)):
                col = pl.multiple_of((part * kv_heads + kv_head) * HEAD_DIM, HEAD_DIM)
                copies.append(pltpu.make_async_copy(block_refs[n].at[:, pl.ds(col, HEAD_DIM)], buf.at[pl.ds(start, span)], sems.at[2 * n + part]))
        for copy in copies:
            copy.start()
        w_copy = pltpu.make_async_copy(w_ref, w_buf, w_sem)
        pl.when(kv_head == 0)(w_copy.start)

        def tile_step(start, masked):
            k_tile = k_buf[pl.ds(start, KEY_TILE)]
            v_tile = v_buf[pl.ds(start, KEY_TILE)]
            for head in range(heads):
                scores = lax.dot_general(q_ref[:, head * HEAD_DIM:(head + 1) * HEAD_DIM], k_tile, (((1,), (1,)), ((), ())), preferred_element_type=jnp.float32)
                if masked:
                    q_pos = row_start + lax.broadcasted_iota(jnp.int32, scores.shape, 0)
                    k_pos = start + lax.broadcasted_iota(jnp.int32, scores.shape, 1)
                    scores = jnp.where(k_pos <= q_pos, scores, MASK_VALUE)
                parts = [scores[:, n:n + 128] for n in range(0, KEY_TILE, 128)]
                new_max = jnp.broadcast_to(jnp.max(functools.reduce(jnp.maximum, parts), axis=1, keepdims=True), (rows, 128))
                if not masked:
                    old_max = m_ref[head]
                    new_max = jnp.maximum(old_max, new_max)
                probs = [jnp.exp2((part - new_max) * SCORE_EXP2) for part in parts]
                tile_sum = functools.reduce(jnp.add, probs)
                weighted = jnp.dot(jnp.concatenate(probs, axis=1).astype(jnp.bfloat16), v_tile, preferred_element_type=jnp.float32)
                if masked:
                    l_ref[head] = tile_sum
                    acc_ref[head] = weighted
                else:
                    rescale = jnp.exp2((old_max - new_max) * SCORE_EXP2)
                    l_ref[head] = l_ref[head] * rescale + tile_sum
                    acc_ref[head] = acc_ref[head] * rescale + weighted
                m_ref[head] = new_max

        for copy in copies[:2]:
            copy.wait()
        own_full = row_start // KEY_TILE
        tile_step(own_full * KEY_TILE, True)
        for copy in copies[2:]:
            copy.wait()
        per_block = span // KEY_TILE
        n_full = own_full + index * per_block
        trips = jnp.maximum(n_full, 1) if ring else n_full
        last = kv_heads - 1

        def full_step(i, carry):
            if ring:
                for step, (head_step, at) in enumerate(((0, 2), (0, 5), (last, 0), (last, 2), (last, 4))):
                    pl.when((kv_head == head_step) & (i == trips * at // 7))(ring.steps[1 + step])

            @pl.when(i < n_full)
            def _():
                tile = jnp.where(i < own_full, i, i - own_full + per_block)
                tile_step(pl.multiple_of(tile * KEY_TILE, KEY_TILE), False)
            return carry

        lax.fori_loop(0, trips, full_step, 0)
        tp_index = lax.axis_index(tp_axis)
        for place, step in enumerate((0, tp_size - 1, 1, 2)):
            take = pl.ds(pl.multiple_of(lax.rem(tp_index + step, tp_size) * piece, piece), piece)
            for head in range(heads):
                col = pl.multiple_of((kv_head * heads + head) * HEAD_DIM, HEAD_DIM)
                total = jnp.sum(l_ref[head, take, :], axis=1, keepdims=True)
                turned[place * piece:(place + 1) * piece, pl.ds(col, HEAD_DIM)] = (acc_ref[head, take, :] / total).astype(jnp.bfloat16)

        @pl.when(kv_head == last)
        def _():
            if ring:
                ring.steps[6]()
            w_copy.wait()

            def part_copy(i):
                cols = pl.ds(pl.multiple_of(i * FF_TILE, FF_TILE), FF_TILE)
                return pltpu.make_async_copy(part_buf.at[:, :, cols], part_ref.at[:, :, cols], part_sem.at[i])

            def project_cols(i, carry):
                cols = pl.ds(pl.multiple_of(i * FF_TILE, FF_TILE), FF_TILE)
                product = jnp.dot(turned[...], w_buf[:, cols], preferred_element_type=jnp.float32)
                for n in range(2 * tp_size):
                    part_buf[n, :, cols] = product[n * half:(n + 1) * half].astype(jnp.bfloat16)
                part_copy(i).start()
                return carry

            lax.fori_loop(0, n_cols, project_cols, 0)
            for i in range(n_cols):
                part_copy(i).wait()
            if ring:
                ring.steps[7]()

    return host(
        kernel, ring, [queries] + blocks + [w_o],
        [pl.BlockSpec((rows, q_cols), lambda i: (chunk, i))] + [pl.BlockSpec(memory_space=pl.ANY)] * 9,
        jax.ShapeDtypeStruct((2 * tp_size, half, dim), jnp.bfloat16), pl.BlockSpec(memory_space=pl.ANY),
        [
            pltpu.VMEM((cp_size * span, HEAD_DIM), jnp.bfloat16),
            pltpu.VMEM((cp_size * span, HEAD_DIM), jnp.bfloat16),
            pltpu.VMEM((heads, rows, 128), jnp.float32),
            pltpu.VMEM((heads, rows, 128), jnp.float32),
            pltpu.VMEM((heads, rows, HEAD_DIM), jnp.float32),
            pltpu.SemaphoreType.DMA((16,)),
            pltpu.VMEM((rows, depth), jnp.bfloat16),
            pltpu.VMEM((depth, dim), jnp.bfloat16),
            pltpu.VMEM((2 * tp_size, half, dim), jnp.bfloat16),
            pltpu.SemaphoreType.DMA,
            pltpu.SemaphoreType.DMA((n_cols,)),
        ],
        (kv_heads,), 4 * rows * q_cols * kv_heads * span * cp_size + 2 * rows * depth * dim,
        4 * kv_heads * cp_size * span * HEAD_DIM + 2 * depth * dim)


def store_pieces(value, ref):
    pieces, half, unused = ref.shape
    for n in range(pieces):
        ref[n] = value[n * half:(n + 1) * half].astype(jnp.bfloat16)


def mlp(pieces, w_gate, w_up, w_down, tile, ring):
    n_pieces, half, dim = pieces.shape
    rows = n_pieces * half
    width = w_gate.shape[1]
    n_up, n_down = width // tile, dim // tile

    def kernel(ins, out_ref, scratch, ring):
        (normed_ref, gate_ref, up_ref, down_ref), (act,) = ins, scratch
        g = pl.program_id(0)
        for step, at in enumerate((0, 2, 4, 6, 8, 9, 12)):
            pl.when(g == at)(ring.steps[step])

        @pl.when(g < n_up)
        def _():
            gate = jnp.dot(normed_ref[...], gate_ref[...], preferred_element_type=jnp.float32)
            up = jnp.dot(normed_ref[...], up_ref[...], preferred_element_type=jnp.float32)
            act[:, pl.ds(pl.multiple_of(g * tile, tile), tile)] = (jax.nn.silu(gate) * up).astype(jnp.bfloat16)

        @pl.when(g >= n_up)
        def _():
            store_pieces(jnp.dot(act[...], down_ref[...], preferred_element_type=jnp.float32), out_ref)

        pl.when(g == n_up + n_down - 1)(ring.finish)

    up_spec = pl.BlockSpec((dim, tile), lambda i: (0, jnp.minimum(i, n_up - 1)))
    return host(
        kernel, ring, [pieces.reshape(rows, dim), w_gate, w_up, w_down],
        [pl.BlockSpec((rows, dim), lambda i: (0, 0), pipeline_mode=pl.Buffered(1)), up_spec, up_spec,
         pl.BlockSpec((width, tile), lambda i: (0, jnp.maximum(i - n_up, 0)))],
        jax.ShapeDtypeStruct((n_pieces, half, dim), jnp.bfloat16), pl.BlockSpec((n_pieces, half, tile), lambda i: (0, 0, jnp.maximum(i - n_up, 0))),
        [pltpu.VMEM((rows, width), jnp.bfloat16)], (n_up + n_down,), 6 * rows * dim * width, 6 * dim * width + 6 * rows * dim)


def all_reduce(ring):
    def body(*refs):
        n_in, n_out = len(ring.operands), len(ring.out_shape)
        ring.bind(refs[:n_in], refs[n_in:n_in + n_out], refs[n_in + n_out:])
        for step in (0, 1, 2, 3, 4, 5, 6, 7):
            ring.steps[step]()

    return pl.pallas_call(body, out_shape=ring.out_shape, in_specs=ring.in_specs, out_specs=ring.out_specs, scratch_shapes=ring.scratch,
                          compiler_params=params(ring))(*ring.operands)


def assemble(chunks, axis, size):
    n_pieces, half, dim = chunks[0].shape
    total = len(chunks) * n_pieces

    def kernel(*refs):
        ins, (out_ref, buf, in_sem, out_sem) = refs[:len(chunks)], refs[len(chunks):]
        index = lax.axis_index(axis)
        places = []
        for n in range(total):
            step = (0, size - 1, 1, 2)[n % n_pieces // 2]
            start = (n // n_pieces * n_pieces + n % 2 + 2 * lax.rem(index + step, size)) * half
            places.append(pl.ds(pl.multiple_of(start, half), half))
        loads = [pltpu.make_async_copy(ins[n // n_pieces].at[n % n_pieces], buf.at[n], in_sem.at[n]) for n in range(total)]
        stores = [pltpu.make_async_copy(buf.at[n], out_ref.at[places[n]], out_sem.at[n]) for n in range(total)]
        for load in loads:
            load.start()
        for load, store in zip(loads, stores):
            load.wait()
            store.start()
        for store in stores:
            store.wait()

    return pl.pallas_call(
        kernel,
        out_shape=jax.ShapeDtypeStruct((total * half, dim), jnp.bfloat16),
        in_specs=[pl.BlockSpec(memory_space=pl.ANY)] * len(chunks),
        out_specs=pl.BlockSpec(memory_space=pl.ANY),
        scratch_shapes=[pltpu.VMEM((total, half, dim), jnp.bfloat16), pltpu.SemaphoreType.DMA((total,)), pltpu.SemaphoreType.DMA((total,))],
        compiler_params=pltpu.CompilerParams(vmem_limit_bytes=VMEM_LIMIT),
        cost_estimate=pl.CostEstimate(flops=0, bytes_accessed=4 * total * half * dim, transcendentals=0),
    )(*chunks)


def permuter(axis, pairs):
    return lambda value: lax.ppermute(value, axis, pairs)


def solution(mesh):
    cp_size = mesh.shape['cp']
    tp_size = mesh.shape['tp']
    row_spec = P(('dp', 'cp'), None)
    cache_spec = P(('dp', 'cp'), 'tp', None)
    col_spec = P(None, 'tp')
    split_rows = P('tp', None)
    vec_spec = P(None)

    def local_layer(x, attn_gain, w_q, w_k, w_v, w_o, mlp_gain, w_gate, w_up, w_down):
        tok_dev = x.shape[0]
        kv_local = w_k.shape[1] // HEAD_DIM
        kv_cols = w_k.shape[1]
        cp_index = lax.axis_index('cp')
        ahead = permuter('cp', [(s, (s + 2) % cp_size) for s in range(cp_size)])
        behind = permuter('cp', [(s, (s - 2) % cp_size) for s in range(cp_size)])
        swap = permuter('cp', [(s, s ^ 1) for s in range(cp_size)])
        cos_tab, sin_tab = rope_tables(cp_index * tok_dev + jnp.arange(tok_dev))
        own = project(kv_kernel, x, attn_gain, cos_tab, sin_tab, [w_k, w_v], 2 * kv_cols)
        middle = tok_dev // 2
        low, high, mate = ahead(own), behind(own), swap(own)
        queries = project(q_kernel, x, attn_gain, cos_tab, sin_tab, [w_q], w_q.shape[1])
        low, high, queries = lax.optimization_barrier((low, high, queries))
        far = jnp.concatenate([ahead(low[:middle]), behind(high[middle:])], axis=0)
        blocks = [own, low, far, high, mate, swap(low), swap(far), swap(high)]
        rows = tok_dev // 2

        def attend(chunk, ring=None):
            return attention(queries, blocks, w_o, chunk, rows, kv_local, 'cp', cp_size, 'tp', tp_size, ring)

        def reduce_over_tp(partial, base, base_row, gain, ring_id):
            return Ring('tp', tp_size, partial, base, base_row, gain, ring_id)

        part0 = attend(0)
        part1, normed0, hidden0 = attend(1, reduce_over_tp(part0, x, 0, mlp_gain, 0))
        down0, normed1, hidden1 = mlp(normed0, w_gate, w_up, w_down, FF_TILE, reduce_over_tp(part1, x, rows, mlp_gain, 1))
        down1, out0 = mlp(normed1, w_gate, w_up, w_down, FF_TILE, reduce_over_tp(down0, hidden0, None, None, 2))
        out1 = all_reduce(reduce_over_tp(down1, hidden1, None, None, 3))[0]
        x_out = assemble([out0, out1], 'tp', tp_size)
        cache_shape = (tok_dev, kv_local, HEAD_DIM)
        return x_out, own[:, :kv_cols].reshape(cache_shape), own[:, kv_cols:].reshape(cache_shape)

    return jax.shard_map(local_layer, mesh=mesh,
                         in_specs=(row_spec, vec_spec, col_spec, col_spec, col_spec, split_rows, vec_spec, col_spec, col_spec, split_rows),
                         out_specs=(row_spec, cache_spec, cache_spec), check_vma=False)
```

```python
import functools
import math
import jax
import jax.numpy as jnp
from jax import lax
from jax.experimental import pallas as pl
from jax.experimental.pallas import tpu as pltpu
from jax.sharding import PartitionSpec as P

HEAD_DIM = 128
ROPE_THETA = 1000000.0
NORM_EPS = 1e-5
MASK_VALUE = -1e30
SCORE_EXP2 = HEAD_DIM ** -0.5 * math.log2(math.e)
KEY_TILE = 1024
ROW_TILE = 256
COL_TILE = 1024
FF_TILE = 512
VMEM_LIMIT = 60 * 1024 * 1024


def rms_norm(rows, gain):
    wide = rows.astype(jnp.float32)
    inv_rms = lax.rsqrt(jnp.mean(wide * wide, axis=-1, keepdims=True) + NORM_EPS)
    return (wide * inv_rms * gain.astype(jnp.float32)).astype(jnp.bfloat16)


def rope_tables(positions):
    inv_freq = jnp.asarray(ROPE_THETA, jnp.float32) ** (-jnp.arange(0, HEAD_DIM, 2, dtype=jnp.float32) / HEAD_DIM)
    angles = positions.astype(jnp.float32)[:, None] * inv_freq[None, :]
    cos, sin = jnp.cos(angles), jnp.sin(angles)
    return jnp.concatenate([cos, cos], axis=-1), jnp.concatenate([-sin, sin], axis=-1)


def rope_head(head, cos_t, sin_t):
    wide = head.astype(jnp.bfloat16).astype(jnp.float32)
    return (wide * cos_t + pltpu.roll(wide, HEAD_DIM // 2, 1) * sin_t).astype(jnp.bfloat16)


def kv_kernel(x_ref, gain_ref, cos_ref, sin_ref, w_k_ref, w_v_ref, kv_ref):
    normed = rms_norm(x_ref[...], gain_ref[...])
    width = w_k_ref.shape[1]
    keys = jnp.dot(normed, w_k_ref[...], preferred_element_type=jnp.float32)
    for head in range(width // HEAD_DIM):
        cols = slice(head * HEAD_DIM, (head + 1) * HEAD_DIM)
        kv_ref[:, cols] = rope_head(keys[:, cols], cos_ref[...], sin_ref[...])
    kv_ref[:, width:] = jnp.dot(normed, w_v_ref[...], preferred_element_type=jnp.float32).astype(jnp.bfloat16)


def q_kernel(x_ref, gain_ref, cos_ref, sin_ref, w_q_ref, q_ref):
    normed = rms_norm(x_ref[...], gain_ref[...])
    queries = jnp.dot(normed, w_q_ref[...], preferred_element_type=jnp.float32)
    for head in range(w_q_ref.shape[1] // HEAD_DIM):
        cols = slice(head * HEAD_DIM, (head + 1) * HEAD_DIM)
        q_ref[:, cols] = rope_head(queries[:, cols], cos_ref[...], sin_ref[...])


def project(kernel, x, gain, cos_tab, sin_tab, weights, out_cols, links=None):
    rows, dim = x.shape
    row_block = lambda cols: pl.BlockSpec((ROW_TILE, cols), lambda i: (i, 0))
    w_cols = sum(w.shape[1] for w in weights)

    def body(ins, out_ref, scratch, links):
        if links:
            pl.when(pl.program_id(0) == 0)(links.begin)
        kernel(*ins, out_ref)
        if links:
            pl.when(pl.program_id(0) == rows // ROW_TILE - 1)(links.finish)

    return host(
        body, links, [x, gain.reshape(1, dim), cos_tab, sin_tab] + weights,
        [row_block(dim), pl.BlockSpec((1, dim), lambda i: (0, 0)), row_block(HEAD_DIM), row_block(HEAD_DIM)]
        + [pl.BlockSpec(w.shape, lambda i: (0, 0), pipeline_mode=pl.Buffered(1)) for w in weights],
        jax.ShapeDtypeStruct((rows, out_cols), jnp.bfloat16), row_block(out_cols), [],
        (rows // ROW_TILE,), 2 * rows * dim * w_cols, 2 * dim * (rows + w_cols))


class Ring:
    n_remote, n_sub = 12, 2

    def __init__(self, axis, size, partial, base, base_row, gain, ring_id):
        self.axis, self.size, self.base_row, self.ring_id = axis, size, base_row, ring_id
        self.pieces, self.half, self.dim = partial.shape
        self.rows = self.half // self.n_sub
        self.normed = gain is not None
        self.operands = [partial, base] + ([gain.reshape(1, self.dim)] if self.normed else [])
        any_spec = pl.BlockSpec(memory_space=pl.ANY)
        self.in_specs = [any_spec, any_spec] + ([pl.BlockSpec(memory_space=pltpu.VMEM)] if self.normed else [])
        shapes = [(self.pieces, self.half, self.dim)] + ([(2, self.half, self.dim)] if self.normed else [])
        self.out_shape = [jax.ShapeDtypeStruct(shape, jnp.bfloat16) for shape in shapes]
        self.out_specs = [any_spec] * len(shapes)
        buf = lambda n: pltpu.VMEM((n, self.half, self.dim), jnp.bfloat16)
        sems = lambda n: pltpu.SemaphoreType.DMA((self.n_sub * n,))
        self.scratch = [buf(6), buf(6), buf(2), sems(self.n_remote), sems(self.n_remote), sems(10)]
        self.steps = [self.begin]
        for kind in (self.pass_on, self.add_up, self.relay):
            self.steps += [functools.partial(kind, sub) for sub in range(self.n_sub)]
        self.steps.append(self.finish)

    def bind(self, ins, outs, scratch):
        partial, base = ins[:2]
        gathered = outs[0]
        arrived, local, sent, self.send_sem, self.recv_sem, self.local_sem = scratch
        index = lax.axis_index(self.axis)
        fwd, back = lax.rem(index + 1, self.size), lax.rem(index + self.size - 1, self.size)
        self.neighbours = (fwd, back)
        self.arrived, self.local, self.sent = arrived, local, sent
        self.gain = ins[2] if self.normed else None
        self.remote, self.copies = [], []
        for sub in range(self.n_sub):
            part = pl.ds(sub * self.rows, self.rows)
            at = lambda ref, n: ref.at[n, part]
            self.remote.append([
                (at(partial, 6), at(arrived, 0), fwd), (at(partial, 7), at(arrived, 1), back),
                (at(partial, 5), at(arrived, 2), fwd), (at(partial, 2), at(arrived, 3), back),
                (at(local, 0), at(arrived, 4), fwd), (at(local, 1), at(arrived, 5), back),
                (at(sent, 0), at(gathered, 2), fwd), (at(sent, 1), at(gathered, 5), back),
                (at(sent, 1), at(gathered, 3), fwd), (at(sent, 0), at(gathered, 4), back),
                (at(gathered, 2), at(gathered, 6), fwd), (at(gathered, 5), at(gathered, 7), back),
            ])
            if self.base_row is None:
                rows = [at(base, 0), at(base, 1)]
            else:
                start = self.base_row + sub * self.rows + index * (2 * self.half)
                rows = [base.at[pl.ds(pl.multiple_of(start + n * self.half, self.rows), self.rows)] for n in range(2)]
            self.copies.append([
                (at(partial, 4), at(local, 0)), (at(partial, 3), at(local, 1)), (at(partial, 0), at(local, 2)), (at(partial, 1), at(local, 3)),
                (rows[0], at(local, 4)), (rows[1], at(local, 5)), (at(sent, 0), at(gathered, 0)), (at(sent, 1), at(gathered, 1)),
            ] + ([(at(local, 4), at(outs[1], 0)), (at(local, 5), at(outs[1], 1))] if self.normed else []))

    def rdma(self, sub, n):
        src, dst, peer = self.remote[sub][n]
        sem = sub * self.n_remote + n
        return pltpu.make_async_remote_copy(src_ref=src, dst_ref=dst, send_sem=self.send_sem.at[sem], recv_sem=self.recv_sem.at[sem],
                                            device_id={self.axis: peer}, device_id_type=pl.DeviceIdType.MESH)

    def copy(self, sub, n):
        src, dst = self.copies[sub][n]
        return pltpu.make_async_copy(src, dst, self.local_sem.at[sub * 10 + n])

    def begin(self):
        barrier = pltpu.get_barrier_semaphore()
        for peer in self.neighbours:
            pl.semaphore_signal(barrier, inc=1, device_id={self.axis: peer}, device_id_type=pl.DeviceIdType.MESH)
        pl.semaphore_wait(barrier, 2)
        for sub in range(self.n_sub):
            for n in range(4):
                self.rdma(sub, n).start()
        for sub in range(self.n_sub):
            for n in range(6):
                self.copy(sub, n).start()

    def pass_on(self, sub):
        part = pl.ds(sub * self.rows, self.rows)
        for n in range(2):
            self.copy(sub, n).wait()
            self.rdma(sub, n).wait_recv()
            self.local[n, part] = (self.local[n, part].astype(jnp.float32) + self.arrived[n, part].astype(jnp.float32)).astype(jnp.bfloat16)
        for n in range(2):
            self.rdma(sub, 4 + n).start()

    def add_up(self, sub):
        part = pl.ds(sub * self.rows, self.rows)
        for n in range(2, 6):
            self.copy(sub, n).wait()
            self.rdma(sub, n).wait_recv()
        for n, (a, b) in enumerate(((4, 3), (2, 5))):
            terms = (self.local[4 + n, part], self.local[2 + n, part], self.arrived[a, part], self.arrived[b, part])
            total = functools.reduce(jnp.add, [term.astype(jnp.float32) for term in terms]).astype(jnp.bfloat16)
            if self.normed:
                self.local[4 + n, part] = total
                self.sent[n, part] = rms_norm(total, self.gain[...])
            else:
                self.sent[n, part] = total
        for n in range(6, 10):
            self.rdma(sub, n).start()
        for n in range(6, len(self.copies[sub])):
            self.copy(sub, n).start()

    def relay(self, sub):
        for n in range(2):
            self.rdma(sub, 6 + n).wait_recv()
            self.rdma(sub, 10 + n).start()

    def finish(self):
        for sub in range(self.n_sub):
            for n in range(8, 12):
                self.rdma(sub, n).wait_recv()
            for n in range(12):
                self.rdma(sub, n).wait_send()
            for n in range(6, len(self.copies[sub])):
                self.copy(sub, n).wait()


class Links:
    def __init__(self, axis, size, operands, n_out, ring_id):
        self.axis, self.size, self.operands, self.ring_id = axis, size, operands, ring_id
        any_spec = pl.BlockSpec(memory_space=pl.ANY)
        self.in_specs = [any_spec] * len(operands)
        self.out_shape = [jax.ShapeDtypeStruct(operands[0].shape, jnp.bfloat16)] * n_out
        self.out_specs = [any_spec] * n_out
        self.scratch = [pltpu.SemaphoreType.DMA((5,)), pltpu.SemaphoreType.DMA((5,))]

    def bind(self, ins, outs, scratch):
        self.ins, self.outs = ins, outs
        self.send_sem, self.recv_sem = scratch
        index = lax.axis_index(self.axis)
        ahead, behind = lax.rem(index + 2, self.size), lax.rem(index + self.size - 2, self.size)
        mate = index + 1 - 2 * lax.rem(index, 2)
        self.neighbours = (ahead, behind, mate)
        if len(ins) == 1:
            self.remote = [(ins[0], outs[0], ahead), (ins[0], outs[1], behind), (ins[0], outs[2], mate)]
        else:
            middle = ins[0].shape[0] // 2
            lower, upper = pl.ds(0, middle), pl.ds(middle, middle)
            self.remote = [
                (ins[0].at[lower], outs[0].at[lower], ahead), (ins[1].at[upper], outs[0].at[upper], behind),
                (ins[0], outs[1], mate), (ins[1], outs[3], mate), (outs[0], outs[2], mate),
            ]

    def rdma(self, n):
        src, dst, peer = self.remote[n]
        return pltpu.make_async_remote_copy(src_ref=src, dst_ref=dst, send_sem=self.send_sem.at[n], recv_sem=self.recv_sem.at[n],
                                            device_id={self.axis: peer}, device_id_type=pl.DeviceIdType.MESH)

    def begin(self):
        barrier = pltpu.get_barrier_semaphore()
        for peer in self.neighbours:
            pl.semaphore_signal(barrier, inc=1, device_id={self.axis: peer}, device_id_type=pl.DeviceIdType.MESH)
        pl.semaphore_wait(barrier, len(self.neighbours))
        for n in range(min(len(self.remote), 4)):
            self.rdma(n).start()

    def finish(self):
        for n in range(len(self.remote)):
            self.rdma(n).wait_send()
            if len(self.remote) == 3:
                self.rdma(n).wait_recv()


def params(ring):
    if ring is None:
        return pltpu.CompilerParams(vmem_limit_bytes=VMEM_LIMIT)
    return pltpu.CompilerParams(vmem_limit_bytes=VMEM_LIMIT, collective_id=ring.ring_id, has_side_effects=True)


def host(kernel, ring, operands, in_specs, out_shape, out_specs, scratch, grid, flops, nbytes):
    n_in, n_ring = len(operands), len(ring.operands) if ring else 0

    def body(*refs):
        ins, rest = refs[:n_in], refs[n_in:]
        ring_ins, rest = rest[:n_ring], rest[n_ring:]
        out, rest = rest[0], rest[1:]
        if ring:
            ring_outs, rest = rest[:len(ring.out_shape)], rest[len(ring.out_shape):]
            ring.bind(ring_ins, ring_outs, rest[len(scratch):])
        kernel(ins, out, rest[:len(scratch)], ring)

    out = pl.pallas_call(
        body,
        out_shape=[out_shape] + (ring.out_shape if ring else []),
        grid=grid,
        in_specs=in_specs + (ring.in_specs if ring else []),
        out_specs=[out_specs] + (ring.out_specs if ring else []),
        scratch_shapes=scratch + (ring.scratch if ring else []),
        compiler_params=params(ring),
        cost_estimate=pl.CostEstimate(flops=flops, bytes_accessed=nbytes, transcendentals=0),
    )(*operands, *(ring.operands if ring else []))
    return out if ring else out[0]


def attention(queries, blocks, w_o, chunk, rows, kv_heads, axis, cp_size, tp_axis, tp_size, ring=None):
    q_cols = queries.shape[1] // kv_heads
    heads = q_cols // HEAD_DIM
    span = blocks[0].shape[0]
    row_start = chunk * rows
    depth, dim = w_o.shape
    piece = rows // tp_size
    half = piece // 2
    n_cols = dim // FF_TILE
    given = [n for n, block in enumerate(blocks) if block is not None]

    def kernel(ins, part_ref, scratch, ring):
        links = ring if isinstance(ring, Links) else None
        ring = None if links else ring
        q_ref, w_ref = ins[0], ins[-1]
        block_refs = dict(zip(given, ins[1:-1]))
        if links:
            block_refs.update(zip((2, 5, 6, 7), links.outs))
        k_buf, v_buf, m_ref, l_ref, acc_ref, sems, turned, w_buf, part_buf, w_sem, part_sem = scratch
        kv_head = pl.program_id(0)
        index = lax.axis_index(axis)
        odd = lax.rem(index, 2)
        if ring or links:
            pl.when(kv_head == 0)((ring or links).begin)
        slots = [0, 2, 4, 6] + [jnp.where(odd == 1, a, b) for a, b in ((1, 7), (3, 1), (5, 3), (7, 5))]
        copies = []
        for n, slot in enumerate(slots):
            start = slot * span if n < 4 else pl.multiple_of(slot * span, span)
            for part, buf in enumerate((k_buf, v_buf)):
                col = pl.multiple_of((part * kv_heads + kv_head) * HEAD_DIM, HEAD_DIM)
                copies.append(pltpu.make_async_copy(block_refs[n].at[:, pl.ds(col, HEAD_DIM)], buf.at[pl.ds(start, span)], sems.at[2 * n + part]))
        late = [2 * n + part for n in (2, 5, 6, 7) for part in range(2)] if links else []
        early = [n for n in range(2, 16) if n not in late]

        def start_late():
            for n in late:
                copies[n].start()

        def wait_late():
            for n in late:
                copies[n].wait()

        def take(arrivals, block_ids):
            for n in arrivals:
                links.rdma(n).wait_recv()
            for n in block_ids:
                for part in range(2):
                    copies[2 * n + part].start()

        def settle(block_ids):
            for n in block_ids:
                for part in range(2):
                    copies[2 * n + part].wait()

        for n in [0, 1] + early:
            copies[n].start()
        if links:
            pl.when(kv_head > 0)(start_late)
        w_copy = pltpu.make_async_copy(w_ref, w_buf, w_sem)
        pl.when(kv_head == 0)(w_copy.start)

        def tile_step(start, masked):
            k_tile = k_buf[pl.ds(start, KEY_TILE)]
            v_tile = v_buf[pl.ds(start, KEY_TILE)]
            for head in range(heads):
                scores = lax.dot_general(q_ref[:, head * HEAD_DIM:(head + 1) * HEAD_DIM], k_tile, (((1,), (1,)), ((), ())), preferred_element_type=jnp.float32)
                if masked:
                    q_pos = row_start + lax.broadcasted_iota(jnp.int32, scores.shape, 0)
                    k_pos = start + lax.broadcasted_iota(jnp.int32, scores.shape, 1)
                    scores = jnp.where(k_pos <= q_pos, scores, MASK_VALUE)
                parts = [scores[:, n:n + 128] for n in range(0, KEY_TILE, 128)]
                new_max = jnp.broadcast_to(jnp.max(functools.reduce(jnp.maximum, parts), axis=1, keepdims=True), (rows, 128))
                if not masked:
                    old_max = m_ref[head]
                    new_max = jnp.maximum(old_max, new_max)
                probs = [jnp.exp2((part - new_max) * SCORE_EXP2) for part in parts]
                tile_sum = functools.reduce(jnp.add, probs)
                weighted = jnp.dot(jnp.concatenate(probs, axis=1).astype(jnp.bfloat16), v_tile, preferred_element_type=jnp.float32)
                if masked:
                    l_ref[head] = tile_sum
                    acc_ref[head] = weighted
                else:
                    rescale = jnp.exp2((old_max - new_max) * SCORE_EXP2)
                    l_ref[head] = l_ref[head] * rescale + tile_sum
                    acc_ref[head] = acc_ref[head] * rescale + weighted
                m_ref[head] = new_max

        for copy in copies[:2]:
            copy.wait()
        own_full = row_start // KEY_TILE
        tile_step(own_full * KEY_TILE, True)
        for n in early:
            copies[n].wait()
        if links:
            pl.when(kv_head > 0)(wait_late)
        per_block = span // KEY_TILE
        n_full = own_full + index * per_block
        trips = 7 * per_block if links else jnp.maximum(n_full, 1) if ring else n_full
        last = kv_heads - 1

        def full_step(i, carry):
            if ring:
                for step, (head_step, at) in enumerate(((0, 2), (0, 5), (last, 0), (last, 2), (last, 4))):
                    pl.when((kv_head == head_step) & (i == trips * at // 7))(ring.steps[1 + step])

            @pl.when(i < n_full)
            def _():
                tile = jnp.where(i < own_full, i, i - own_full + per_block)
                tile_step(pl.multiple_of(tile * KEY_TILE, KEY_TILE), False)
            return carry

        def arrival_step(i, carry):
            place = i // per_block

            def far_here():
                take((0, 1), (2,))
                links.rdma(4).start()
                settle((2,))

            def mates_here():
                take((2, 3), (5, 7))
                settle((5, 7))

            def far_mate_here():
                take((4,), (6,))
                settle((6,))

            for at, action in ((3, mates_here), (4, far_here), (6, far_mate_here)):
                pl.when((kv_head == 0) & (i == at * per_block))(action)
            slot = jnp.int32(0)
            for n, (a, b) in enumerate(((2, 2), (6, 6), (1, 7), (3, 1), (7, 5), (4, 4), (5, 3))):
                slot = jnp.where(place == n, jnp.where(odd == 1, a, b), slot)

            @pl.when(slot <= index)
            def _():
                tile_step(pl.multiple_of(slot * span + lax.rem(i, per_block) * KEY_TILE, KEY_TILE), False)
            return carry

        lax.fori_loop(0, trips, arrival_step if links else full_step, 0)
        tp_index = lax.axis_index(tp_axis)
        for place, step in enumerate((0, tp_size - 1, 1, 2)):
            from_rows = pl.ds(pl.multiple_of(lax.rem(tp_index + step, tp_size) * piece, piece), piece)
            for head in range(heads):
                col = pl.multiple_of((kv_head * heads + head) * HEAD_DIM, HEAD_DIM)
                total = jnp.sum(l_ref[head, from_rows, :], axis=1, keepdims=True)
                turned[place * piece:(place + 1) * piece, pl.ds(col, HEAD_DIM)] = (acc_ref[head, from_rows, :] / total).astype(jnp.bfloat16)

        @pl.when(kv_head == last)
        def _():
            if ring:
                ring.steps[6]()
            w_copy.wait()

            def part_copy(i):
                cols = pl.ds(pl.multiple_of(i * FF_TILE, FF_TILE), FF_TILE)
                return pltpu.make_async_copy(part_buf.at[:, :, cols], part_ref.at[:, :, cols], part_sem.at[i])

            def project_cols(i, carry):
                cols = pl.ds(pl.multiple_of(i * FF_TILE, FF_TILE), FF_TILE)
                product = jnp.dot(turned[...], w_buf[:, cols], preferred_element_type=jnp.float32)
                for n in range(2 * tp_size):
                    part_buf[n, :, cols] = product[n * half:(n + 1) * half].astype(jnp.bfloat16)
                part_copy(i).start()
                return carry

            lax.fori_loop(0, n_cols, project_cols, 0)
            for i in range(n_cols):
                part_copy(i).wait()
            if ring or links:
                (ring or links).finish()

    return host(
        kernel, ring, [queries] + [blocks[n] for n in given] + [w_o],
        [pl.BlockSpec((rows, q_cols), lambda i: (chunk, i))] + [pl.BlockSpec(memory_space=pl.ANY)] * (len(given) + 1),
        jax.ShapeDtypeStruct((2 * tp_size, half, dim), jnp.bfloat16), pl.BlockSpec(memory_space=pl.ANY),
        [
            pltpu.VMEM((cp_size * span, HEAD_DIM), jnp.bfloat16),
            pltpu.VMEM((cp_size * span, HEAD_DIM), jnp.bfloat16),
            pltpu.VMEM((heads, rows, 128), jnp.float32),
            pltpu.VMEM((heads, rows, 128), jnp.float32),
            pltpu.VMEM((heads, rows, HEAD_DIM), jnp.float32),
            pltpu.SemaphoreType.DMA((16,)),
            pltpu.VMEM((rows, depth), jnp.bfloat16),
            pltpu.VMEM((depth, dim), jnp.bfloat16),
            pltpu.VMEM((2 * tp_size, half, dim), jnp.bfloat16),
            pltpu.SemaphoreType.DMA,
            pltpu.SemaphoreType.DMA((n_cols,)),
        ],
        (kv_heads,), 4 * rows * q_cols * kv_heads * span * cp_size + 2 * rows * depth * dim,
        4 * kv_heads * cp_size * span * HEAD_DIM + 2 * depth * dim)


def store_pieces(value, ref):
    pieces, half, unused = ref.shape
    for n in range(pieces):
        ref[n] = value[n * half:(n + 1) * half].astype(jnp.bfloat16)


def mlp(pieces, w_gate, w_up, w_down, tile, ring):
    n_pieces, half, dim = pieces.shape
    rows = n_pieces * half
    width = w_gate.shape[1]
    n_up, n_down = width // tile, dim // tile

    def kernel(ins, out_ref, scratch, ring):
        (pieces_ref, gate_ref, up_ref, down_ref), (act, normed_ref, row_sem) = ins, scratch
        g = pl.program_id(0)
        for step, at in enumerate((0, 2, 4, 6, 8, 9, 12)):
            pl.when(g == at)(ring.steps[step])

        @pl.when(g == 0)
        def _():
            rows_copy = pltpu.make_async_copy(pieces_ref, normed_ref, row_sem)
            rows_copy.start()
            rows_copy.wait()

        @pl.when(g < n_up)
        def _():
            gate = jnp.dot(normed_ref[...], gate_ref[...], preferred_element_type=jnp.float32)
            up = jnp.dot(normed_ref[...], up_ref[...], preferred_element_type=jnp.float32)
            act[:, pl.ds(pl.multiple_of(g * tile, tile), tile)] = (jax.nn.silu(gate) * up).astype(jnp.bfloat16)

        @pl.when(g >= n_up)
        def _():
            store_pieces(jnp.dot(act[...], down_ref[...], preferred_element_type=jnp.float32), out_ref)

        pl.when(g == n_up + n_down - 1)(ring.finish)

    up_spec = pl.BlockSpec((dim, tile), lambda i: (0, jnp.minimum(i, n_up - 1)))
    return host(
        kernel, ring, [pieces.reshape(rows, dim), w_gate, w_up, w_down],
        [pl.BlockSpec(memory_space=pl.ANY), up_spec, up_spec,
         pl.BlockSpec((width, tile), lambda i: (0, jnp.maximum(i - n_up, 0)))],
        jax.ShapeDtypeStruct((n_pieces, half, dim), jnp.bfloat16), pl.BlockSpec((n_pieces, half, tile), lambda i: (0, 0, jnp.maximum(i - n_up, 0))),
        [pltpu.VMEM((rows, width), jnp.bfloat16), pltpu.VMEM((rows, dim), jnp.bfloat16), pltpu.SemaphoreType.DMA], (n_up + n_down,), 6 * rows * dim * width, 6 * dim * width + 6 * rows * dim)


def all_reduce(ring):
    def body(*refs):
        n_in, n_out = len(ring.operands), len(ring.out_shape)
        ring.bind(refs[:n_in], refs[n_in:n_in + n_out], refs[n_in + n_out:])
        for step in (0, 1, 2, 3, 4, 5, 6, 7):
            ring.steps[step]()

    return pl.pallas_call(body, out_shape=ring.out_shape, in_specs=ring.in_specs, out_specs=ring.out_specs, scratch_shapes=ring.scratch,
                          compiler_params=params(ring))(*ring.operands)


def assemble(chunks, axis, size):
    n_pieces, half, dim = chunks[0].shape
    total = len(chunks) * n_pieces

    def kernel(*refs):
        ins, (out_ref, buf, in_sem, out_sem) = refs[:len(chunks)], refs[len(chunks):]
        index = lax.axis_index(axis)
        places = []
        for n in range(total):
            step = (0, size - 1, 1, 2)[n % n_pieces // 2]
            start = (n // n_pieces * n_pieces + n % 2 + 2 * lax.rem(index + step, size)) * half
            places.append(pl.ds(pl.multiple_of(start, half), half))
        loads = [pltpu.make_async_copy(ins[n // n_pieces].at[n % n_pieces], buf.at[n], in_sem.at[n]) for n in range(total)]
        stores = [pltpu.make_async_copy(buf.at[n], out_ref.at[places[n]], out_sem.at[n]) for n in range(total)]
        for load in loads:
            load.start()
        for load, store in zip(loads, stores):
            load.wait()
            store.start()
        for store in stores:
            store.wait()

    return pl.pallas_call(
        kernel,
        out_shape=jax.ShapeDtypeStruct((total * half, dim), jnp.bfloat16),
        in_specs=[pl.BlockSpec(memory_space=pl.ANY)] * len(chunks),
        out_specs=pl.BlockSpec(memory_space=pl.ANY),
        scratch_shapes=[pltpu.VMEM((total, half, dim), jnp.bfloat16), pltpu.SemaphoreType.DMA((total,)), pltpu.SemaphoreType.DMA((total,))],
        compiler_params=pltpu.CompilerParams(vmem_limit_bytes=VMEM_LIMIT),
        cost_estimate=pl.CostEstimate(flops=0, bytes_accessed=4 * total * half * dim, transcendentals=0),
    )(*chunks)


def solution(mesh):
    cp_size = mesh.shape['cp']
    tp_size = mesh.shape['tp']
    row_spec = P(('dp', 'cp'), None)
    cache_spec = P(('dp', 'cp'), 'tp', None)
    col_spec = P(None, 'tp')
    split_rows = P('tp', None)
    vec_spec = P(None)

    def local_layer(x, attn_gain, w_q, w_k, w_v, w_o, mlp_gain, w_gate, w_up, w_down):
        tok_dev = x.shape[0]
        kv_local = w_k.shape[1] // HEAD_DIM
        kv_cols = w_k.shape[1]
        cp_index = lax.axis_index('cp')
        cos_tab, sin_tab = rope_tables(cp_index * tok_dev + jnp.arange(tok_dev))
        own = project(kv_kernel, x, attn_gain, cos_tab, sin_tab, [w_k, w_v], 2 * kv_cols)
        queries, low, high, mate = project(q_kernel, x, attn_gain, cos_tab, sin_tab, [w_q], w_q.shape[1], Links('cp', cp_size, [own], 3, 4))
        blocks = [own, low, None, high, mate, None, None, None]
        rows = tok_dev // 2

        def attend(chunk, ring=None):
            return attention(queries, blocks, w_o, chunk, rows, kv_local, 'cp', cp_size, 'tp', tp_size, ring)

        def reduce_over_tp(partial, base, base_row, gain, ring_id):
            return Ring('tp', tp_size, partial, base, base_row, gain, ring_id)

        part0, far, mate_low, mate_far, mate_high = attend(0, Links('cp', cp_size, [low, high], 4, 5))
        blocks = [own, low, far, high, mate, mate_low, mate_far, mate_high]
        part1, normed0, hidden0 = attend(1, reduce_over_tp(part0, x, 0, mlp_gain, 0))
        down0, normed1, hidden1 = mlp(normed0, w_gate, w_up, w_down, FF_TILE, reduce_over_tp(part1, x, rows, mlp_gain, 1))
        down1, out0 = mlp(normed1, w_gate, w_up, w_down, FF_TILE, reduce_over_tp(down0, hidden0, None, None, 2))
        out1 = all_reduce(reduce_over_tp(down1, hidden1, None, None, 3))[0]
        x_out = assemble([out0, out1], 'tp', tp_size)
        cache_shape = (tok_dev, kv_local, HEAD_DIM)
        return x_out, own[:, :kv_cols].reshape(cache_shape), own[:, kv_cols:].reshape(cache_shape)

    return jax.shard_map(local_layer, mesh=mesh,
                         in_specs=(row_spec, vec_spec, col_spec, col_spec, col_spec, split_rows, vec_spec, col_spec, col_spec, split_rows),
                         out_specs=(row_spec, cache_spec, cache_spec), check_vma=False)
```

```python
import functools
import math
import jax
import jax.numpy as jnp
from jax import lax
from jax.experimental import pallas as pl
from jax.experimental.pallas import tpu as pltpu
from jax.sharding import PartitionSpec as P

HEAD_DIM = 128
ROPE_THETA = 1000000.0
NORM_EPS = 1e-5
MASK_VALUE = -1e30
SCORE_EXP2 = HEAD_DIM ** -0.5 * math.log2(math.e)
KEY_TILE = 1024
ROW_TILE = 256
COL_TILE = 1024
FF_TILE = 512
VMEM_LIMIT = 60 * 1024 * 1024


def rms_norm(rows, gain):
    wide = rows.astype(jnp.float32)
    inv_rms = lax.rsqrt(jnp.mean(wide * wide, axis=-1, keepdims=True) + NORM_EPS)
    return (wide * inv_rms * gain.astype(jnp.float32)).astype(jnp.bfloat16)


def rope_tables(positions):
    inv_freq = jnp.asarray(ROPE_THETA, jnp.float32) ** (-jnp.arange(0, HEAD_DIM, 2, dtype=jnp.float32) / HEAD_DIM)
    angles = positions.astype(jnp.float32)[:, None] * inv_freq[None, :]
    cos, sin = jnp.cos(angles), jnp.sin(angles)
    return jnp.concatenate([cos, cos], axis=-1), jnp.concatenate([-sin, sin], axis=-1)


def rope_head(head, cos_t, sin_t):
    wide = head.astype(jnp.bfloat16).astype(jnp.float32)
    return (wide * cos_t + pltpu.roll(wide, HEAD_DIM // 2, 1) * sin_t).astype(jnp.bfloat16)


def project(x, gain, cos_tab, sin_tab, w_k, w_v, w_q, links):
    rows, dim = x.shape
    width, q_cols = w_k.shape[1], w_q.shape[1]
    n_tiles = rows // ROW_TILE

    def kernel(ins, q_ref, scratch, links):
        (x_ref, gain_ref, cos_ref, sin_ref, w_k_ref, w_v_ref, w_q_ref), (own,) = ins, scratch
        g = pl.program_id(0)
        kv_out = links.outs[3]
        links.source(own, ROW_TILE)
        pl.when(g == 0)(links.begin)

        def send(tile):
            for n in range(3):
                links.rdma(3 * tile + n).start()

        for tile in range(n_tiles):
            pl.when(g == tile + 1)(functools.partial(send, tile))
        store = pltpu.make_async_copy(own, kv_out, links.local_sem)
        pl.when(g == n_tiles)(store.start)
        normed = rms_norm(x_ref[...], gain_ref[...])

        @pl.when(g < n_tiles)
        def _():
            tile = pl.ds(pl.multiple_of(g * ROW_TILE, ROW_TILE), ROW_TILE)
            keys = jnp.dot(normed, w_k_ref[...], preferred_element_type=jnp.float32)
            for head in range(width // HEAD_DIM):
                cols = slice(head * HEAD_DIM, (head + 1) * HEAD_DIM)
                own[tile, cols] = rope_head(keys[:, cols], cos_ref[...], sin_ref[...])
            own[tile, width:] = jnp.dot(normed, w_v_ref[...], preferred_element_type=jnp.float32).astype(jnp.bfloat16)

        @pl.when(g >= n_tiles)
        def _():
            queries = jnp.dot(normed, w_q_ref[...], preferred_element_type=jnp.float32)
            for head in range(q_cols // HEAD_DIM):
                cols = slice(head * HEAD_DIM, (head + 1) * HEAD_DIM)
                q_ref[:, cols] = rope_head(queries[:, cols], cos_ref[...], sin_ref[...])

        @pl.when(g == 2 * n_tiles - 1)
        def _():
            links.finish()
            store.wait()

    row_block = lambda cols: pl.BlockSpec((ROW_TILE, cols), lambda i: (lax.rem(i, n_tiles), 0))
    weights = [w_k, w_v, w_q]
    return host(
        kernel, links, [x, gain.reshape(1, dim), cos_tab, sin_tab] + weights,
        [row_block(dim), pl.BlockSpec((1, dim), lambda i: (0, 0)), row_block(HEAD_DIM), row_block(HEAD_DIM)]
        + [pl.BlockSpec(w.shape, lambda i: (0, 0), pipeline_mode=pl.Buffered(1)) for w in weights],
        jax.ShapeDtypeStruct((rows, q_cols), jnp.bfloat16), pl.BlockSpec((ROW_TILE, q_cols), lambda i: (jnp.maximum(i - n_tiles, 0), 0)),
        [pltpu.VMEM((rows, 2 * width), jnp.bfloat16)],
        (2 * n_tiles,), 2 * rows * dim * (2 * width + q_cols), 2 * dim * (2 * rows + 2 * width + q_cols))


class Ring:
    n_remote, n_sub = 12, 2

    def __init__(self, axis, size, partial, base, base_row, gain, ring_id):
        self.axis, self.size, self.base_row, self.ring_id = axis, size, base_row, ring_id
        self.pieces, self.half, self.dim = partial.shape
        self.rows = self.half // self.n_sub
        self.normed = gain is not None
        self.operands = [partial, base] + ([gain.reshape(1, self.dim)] if self.normed else [])
        any_spec = pl.BlockSpec(memory_space=pl.ANY)
        self.in_specs = [any_spec, any_spec] + ([pl.BlockSpec(memory_space=pltpu.VMEM)] if self.normed else [])
        shapes = [(self.pieces, self.half, self.dim)] + ([(2, self.half, self.dim)] if self.normed else [])
        self.out_shape = [jax.ShapeDtypeStruct(shape, jnp.bfloat16) for shape in shapes]
        self.out_specs = [any_spec] * len(shapes)
        buf = lambda n: pltpu.VMEM((n, self.half, self.dim), jnp.bfloat16)
        sems = lambda n: pltpu.SemaphoreType.DMA((self.n_sub * n,))
        self.scratch = [buf(6), buf(6), buf(2), sems(self.n_remote), sems(self.n_remote), sems(10)]
        self.steps = [self.begin]
        for kind in (self.pass_on, self.add_up, self.relay):
            self.steps += [functools.partial(kind, sub) for sub in range(self.n_sub)]
        self.steps.append(self.finish)

    def bind(self, ins, outs, scratch):
        partial, base = ins[:2]
        gathered = outs[0]
        arrived, local, sent, self.send_sem, self.recv_sem, self.local_sem = scratch
        index = lax.axis_index(self.axis)
        fwd, back = lax.rem(index + 1, self.size), lax.rem(index + self.size - 1, self.size)
        self.neighbours = (fwd, back)
        self.arrived, self.local, self.sent = arrived, local, sent
        self.gain = ins[2] if self.normed else None
        self.remote, self.copies = [], []
        for sub in range(self.n_sub):
            part = pl.ds(sub * self.rows, self.rows)
            at = lambda ref, n: ref.at[n, part]
            self.remote.append([
                (at(partial, 6), at(arrived, 0), fwd), (at(partial, 7), at(arrived, 1), back),
                (at(partial, 5), at(arrived, 2), fwd), (at(partial, 2), at(arrived, 3), back),
                (at(local, 0), at(arrived, 4), fwd), (at(local, 1), at(arrived, 5), back),
                (at(sent, 0), at(gathered, 2), fwd), (at(sent, 1), at(gathered, 5), back),
                (at(sent, 1), at(gathered, 3), fwd), (at(sent, 0), at(gathered, 4), back),
                (at(gathered, 2), at(gathered, 6), fwd), (at(gathered, 5), at(gathered, 7), back),
            ])
            if self.base_row is None:
                rows = [at(base, 0), at(base, 1)]
            else:
                start = self.base_row + sub * self.rows + index * (2 * self.half)
                rows = [base.at[pl.ds(pl.multiple_of(start + n * self.half, self.rows), self.rows)] for n in range(2)]
            self.copies.append([
                (at(partial, 4), at(local, 0)), (at(partial, 3), at(local, 1)), (at(partial, 0), at(local, 2)), (at(partial, 1), at(local, 3)),
                (rows[0], at(local, 4)), (rows[1], at(local, 5)), (at(sent, 0), at(gathered, 0)), (at(sent, 1), at(gathered, 1)),
            ] + ([(at(local, 4), at(outs[1], 0)), (at(local, 5), at(outs[1], 1))] if self.normed else []))

    def rdma(self, sub, n):
        src, dst, peer = self.remote[sub][n]
        sem = sub * self.n_remote + n
        return pltpu.make_async_remote_copy(src_ref=src, dst_ref=dst, send_sem=self.send_sem.at[sem], recv_sem=self.recv_sem.at[sem],
                                            device_id={self.axis: peer}, device_id_type=pl.DeviceIdType.MESH)

    def copy(self, sub, n):
        src, dst = self.copies[sub][n]
        return pltpu.make_async_copy(src, dst, self.local_sem.at[sub * 10 + n])

    def begin(self):
        barrier = pltpu.get_barrier_semaphore()
        for peer in self.neighbours:
            pl.semaphore_signal(barrier, inc=1, device_id={self.axis: peer}, device_id_type=pl.DeviceIdType.MESH)
        pl.semaphore_wait(barrier, 2)
        for sub in range(self.n_sub):
            for n in range(4):
                self.rdma(sub, n).start()
        for sub in range(self.n_sub):
            for n in range(6):
                self.copy(sub, n).start()

    def pass_on(self, sub):
        part = pl.ds(sub * self.rows, self.rows)
        for n in range(2):
            self.copy(sub, n).wait()
            self.rdma(sub, n).wait_recv()
            self.local[n, part] = (self.local[n, part].astype(jnp.float32) + self.arrived[n, part].astype(jnp.float32)).astype(jnp.bfloat16)
        for n in range(2):
            self.rdma(sub, 4 + n).start()

    def add_up(self, sub):
        part = pl.ds(sub * self.rows, self.rows)
        for n in range(2, 6):
            self.copy(sub, n).wait()
            self.rdma(sub, n).wait_recv()
        for n, (a, b) in enumerate(((4, 3), (2, 5))):
            terms = (self.local[4 + n, part], self.local[2 + n, part], self.arrived[a, part], self.arrived[b, part])
            total = functools.reduce(jnp.add, [term.astype(jnp.float32) for term in terms]).astype(jnp.bfloat16)
            if self.normed:
                self.local[4 + n, part] = total
                self.sent[n, part] = rms_norm(total, self.gain[...])
            else:
                self.sent[n, part] = total
        for n in range(6, 10):
            self.rdma(sub, n).start()
        for n in range(6, len(self.copies[sub])):
            self.copy(sub, n).start()

    def relay(self, sub):
        for n in range(2):
            self.rdma(sub, 6 + n).wait_recv()
            self.rdma(sub, 10 + n).start()

    def finish(self):
        for sub in range(self.n_sub):
            for n in range(8, 12):
                self.rdma(sub, n).wait_recv()
            for n in range(12):
                self.rdma(sub, n).wait_send()
            for n in range(6, len(self.copies[sub])):
                self.copy(sub, n).wait()


class Links:
    def __init__(self, axis, size, operands, block, n_out, ring_id):
        self.axis, self.size, self.operands, self.ring_id = axis, size, operands, ring_id
        any_spec = pl.BlockSpec(memory_space=pl.ANY)
        self.in_specs = [any_spec] * len(operands)
        self.out_shape = [jax.ShapeDtypeStruct(block, jnp.bfloat16)] * n_out
        self.out_specs = [any_spec] * n_out
        self.scratch = [pltpu.SemaphoreType.DMA((12,)), pltpu.SemaphoreType.DMA((12,)), pltpu.SemaphoreType.DMA]

    def bind(self, ins, outs, scratch):
        self.ins, self.outs = ins, outs
        self.send_sem, self.recv_sem, self.local_sem = scratch
        index = lax.axis_index(self.axis)
        ahead, behind = lax.rem(index + 2, self.size), lax.rem(index + self.size - 2, self.size)
        mate = index + 1 - 2 * lax.rem(index, 2)
        self.neighbours = (ahead, behind, mate)
        if ins:
            middle = ins[0].shape[0] // 2
            lower, upper = pl.ds(0, middle), pl.ds(middle, middle)
            self.remote = [
                (ins[0].at[lower], outs[0].at[lower], ahead), (ins[1].at[upper], outs[0].at[upper], behind),
                (ins[0], outs[1], mate), (ins[1], outs[3], mate), (outs[0], outs[2], mate),
            ]

    def rdma(self, n):
        src, dst, peer = self.remote[n]
        return pltpu.make_async_remote_copy(src_ref=src, dst_ref=dst, send_sem=self.send_sem.at[n], recv_sem=self.recv_sem.at[n],
                                            device_id={self.axis: peer}, device_id_type=pl.DeviceIdType.MESH)

    def begin(self):
        barrier = pltpu.get_barrier_semaphore()
        for peer in self.neighbours:
            pl.semaphore_signal(barrier, inc=1, device_id={self.axis: peer}, device_id_type=pl.DeviceIdType.MESH)
        pl.semaphore_wait(barrier, len(self.neighbours))
        if self.ins:
            for n in range(4):
                self.rdma(n).start()

    def source(self, own, tile_rows):
        self.remote = [(own.at[pl.ds(n, tile_rows)], out.at[pl.ds(n, tile_rows)], peer)
                       for n in range(0, own.shape[0], tile_rows) for out, peer in zip(self.outs, self.neighbours)]

    def finish(self):
        for n in range(len(self.remote)):
            self.rdma(n).wait_send()
            if not self.ins:
                self.rdma(n).wait_recv()


def params(ring):
    if ring is None:
        return pltpu.CompilerParams(vmem_limit_bytes=VMEM_LIMIT)
    return pltpu.CompilerParams(vmem_limit_bytes=VMEM_LIMIT, collective_id=ring.ring_id, has_side_effects=True)


def host(kernel, ring, operands, in_specs, out_shape, out_specs, scratch, grid, flops, nbytes):
    n_in, n_ring = len(operands), len(ring.operands) if ring else 0

    def body(*refs):
        ins, rest = refs[:n_in], refs[n_in:]
        ring_ins, rest = rest[:n_ring], rest[n_ring:]
        out, rest = rest[0], rest[1:]
        if ring:
            ring_outs, rest = rest[:len(ring.out_shape)], rest[len(ring.out_shape):]
            ring.bind(ring_ins, ring_outs, rest[len(scratch):])
        kernel(ins, out, rest[:len(scratch)], ring)

    out = pl.pallas_call(
        body,
        out_shape=[out_shape] + (ring.out_shape if ring else []),
        grid=grid,
        in_specs=in_specs + (ring.in_specs if ring else []),
        out_specs=[out_specs] + (ring.out_specs if ring else []),
        scratch_shapes=scratch + (ring.scratch if ring else []),
        compiler_params=params(ring),
        cost_estimate=pl.CostEstimate(flops=flops, bytes_accessed=nbytes, transcendentals=0),
    )(*operands, *(ring.operands if ring else []))
    return out if ring else out[0]


def attention(queries, blocks, w_o, chunk, rows, kv_heads, axis, cp_size, tp_axis, tp_size, ring=None):
    q_cols = queries.shape[1] // kv_heads
    heads = q_cols // HEAD_DIM
    span = blocks[0].shape[0]
    row_start = chunk * rows
    depth, dim = w_o.shape
    piece = rows // tp_size
    half = piece // 2
    n_cols = dim // FF_TILE
    given = [n for n, block in enumerate(blocks) if block is not None]

    def kernel(ins, part_ref, scratch, ring):
        links = ring if isinstance(ring, Links) else None
        ring = None if links else ring
        q_ref, w_ref = ins[0], ins[-1]
        block_refs = dict(zip(given, ins[1:-1]))
        if links:
            block_refs.update(zip((2, 5, 6, 7), links.outs))
        k_buf, v_buf, m_ref, l_ref, acc_ref, sems, turned, w_buf, part_buf, w_sem, part_sem = scratch
        kv_head = pl.program_id(0)
        index = lax.axis_index(axis)
        odd = lax.rem(index, 2)
        if ring or links:
            pl.when(kv_head == 0)((ring or links).begin)
        slots = [0, 2, 4, 6] + [jnp.where(odd == 1, a, b) for a, b in ((1, 7), (3, 1), (5, 3), (7, 5))]
        copies = []
        for n, slot in enumerate(slots):
            start = slot * span if n < 4 else pl.multiple_of(slot * span, span)
            for part, buf in enumerate((k_buf, v_buf)):
                col = pl.multiple_of((part * kv_heads + kv_head) * HEAD_DIM, HEAD_DIM)
                copies.append(pltpu.make_async_copy(block_refs[n].at[:, pl.ds(col, HEAD_DIM)], buf.at[pl.ds(start, span)], sems.at[2 * n + part]))
        late = [2 * n + part for n in (2, 5, 6, 7) for part in range(2)] if links else []
        early = [n for n in range(2, 16) if n not in late]

        def start_late():
            for n in late:
                copies[n].start()

        def wait_late():
            for n in late:
                copies[n].wait()

        def take(arrivals, block_ids):
            for n in arrivals:
                links.rdma(n).wait_recv()
            for n in block_ids:
                for part in range(2):
                    copies[2 * n + part].start()

        def settle(block_ids):
            for n in block_ids:
                for part in range(2):
                    copies[2 * n + part].wait()

        for n in [0, 1] + early:
            copies[n].start()
        if links:
            pl.when(kv_head > 0)(start_late)
        w_copy = pltpu.make_async_copy(w_ref, w_buf, w_sem)
        pl.when(kv_head == 0)(w_copy.start)

        def tile_step(start, masked):
            k_tile = k_buf[pl.ds(start, KEY_TILE)]
            v_tile = v_buf[pl.ds(start, KEY_TILE)]
            for head in range(heads):
                scores = lax.dot_general(q_ref[:, head * HEAD_DIM:(head + 1) * HEAD_DIM], k_tile, (((1,), (1,)), ((), ())), preferred_element_type=jnp.float32)
                if masked:
                    q_pos = row_start + lax.broadcasted_iota(jnp.int32, scores.shape, 0)
                    k_pos = start + lax.broadcasted_iota(jnp.int32, scores.shape, 1)
                    scores = jnp.where(k_pos <= q_pos, scores, MASK_VALUE)
                parts = [scores[:, n:n + 128] for n in range(0, KEY_TILE, 128)]
                new_max = jnp.broadcast_to(jnp.max(functools.reduce(jnp.maximum, parts), axis=1, keepdims=True), (rows, 128))
                if not masked:
                    old_max = m_ref[head]
                    new_max = jnp.maximum(old_max, new_max)
                probs = [jnp.exp2((part - new_max) * SCORE_EXP2) for part in parts]
                tile_sum = functools.reduce(jnp.add, probs)
                weighted = jnp.dot(jnp.concatenate(probs, axis=1).astype(jnp.bfloat16), v_tile, preferred_element_type=jnp.float32)
                if masked:
                    l_ref[head] = tile_sum
                    acc_ref[head] = weighted
                else:
                    rescale = jnp.exp2((old_max - new_max) * SCORE_EXP2)
                    l_ref[head] = l_ref[head] * rescale + tile_sum
                    acc_ref[head] = acc_ref[head] * rescale + weighted
                m_ref[head] = new_max

        for copy in copies[:2]:
            copy.wait()
        own_full = row_start // KEY_TILE
        tile_step(own_full * KEY_TILE, True)
        for n in early:
            copies[n].wait()
        if links:
            pl.when(kv_head > 0)(wait_late)
        per_block = span // KEY_TILE
        n_full = own_full + index * per_block
        trips = 7 * per_block if links else jnp.maximum(n_full, 1) if ring else n_full
        last = kv_heads - 1

        def full_step(i, carry):
            if ring:
                for step, (head_step, at) in enumerate(((0, 2), (0, 5), (last, 0), (last, 2), (last, 4))):
                    pl.when((kv_head == head_step) & (i == trips * at // 7))(ring.steps[1 + step])

            @pl.when(i < n_full)
            def _():
                tile = jnp.where(i < own_full, i, i - own_full + per_block)
                tile_step(pl.multiple_of(tile * KEY_TILE, KEY_TILE), False)
            return carry

        def arrival_step(i, carry):
            place = i // per_block

            def far_here():
                take((0, 1), (2,))
                links.rdma(4).start()
                settle((2,))

            def mates_here():
                take((2, 3), (5, 7))
                settle((5, 7))

            def far_mate_here():
                take((4,), (6,))
                settle((6,))

            for at, action in ((3, mates_here), (4, far_here), (6, far_mate_here)):
                pl.when((kv_head == 0) & (i == at * per_block))(action)
            slot = jnp.int32(0)
            for n, (a, b) in enumerate(((2, 2), (6, 6), (1, 7), (3, 1), (7, 5), (4, 4), (5, 3))):
                slot = jnp.where(place == n, jnp.where(odd == 1, a, b), slot)

            @pl.when(slot <= index)
            def _():
                tile_step(pl.multiple_of(slot * span + lax.rem(i, per_block) * KEY_TILE, KEY_TILE), False)
            return carry

        lax.fori_loop(0, trips, arrival_step if links else full_step, 0)
        tp_index = lax.axis_index(tp_axis)
        for place, step in enumerate((0, tp_size - 1, 1, 2)):
            from_rows = pl.ds(pl.multiple_of(lax.rem(tp_index + step, tp_size) * piece, piece), piece)
            for head in range(heads):
                col = pl.multiple_of((kv_head * heads + head) * HEAD_DIM, HEAD_DIM)
                total = jnp.sum(l_ref[head, from_rows, :], axis=1, keepdims=True)
                turned[place * piece:(place + 1) * piece, pl.ds(col, HEAD_DIM)] = (acc_ref[head, from_rows, :] / total).astype(jnp.bfloat16)

        @pl.when(kv_head == last)
        def _():
            if ring:
                ring.steps[6]()
            w_copy.wait()

            def part_copy(i):
                cols = pl.ds(pl.multiple_of(i * FF_TILE, FF_TILE), FF_TILE)
                return pltpu.make_async_copy(part_buf.at[:, :, cols], part_ref.at[:, :, cols], part_sem.at[i])

            def project_cols(i, carry):
                cols = pl.ds(pl.multiple_of(i * FF_TILE, FF_TILE), FF_TILE)
                product = jnp.dot(turned[...], w_buf[:, cols], preferred_element_type=jnp.float32)
                for n in range(2 * tp_size):
                    part_buf[n, :, cols] = product[n * half:(n + 1) * half].astype(jnp.bfloat16)
                part_copy(i).start()
                return carry

            lax.fori_loop(0, n_cols, project_cols, 0)
            for i in range(n_cols):
                part_copy(i).wait()
            if ring or links:
                (ring or links).finish()

    return host(
        kernel, ring, [queries] + [blocks[n] for n in given] + [w_o],
        [pl.BlockSpec((rows, q_cols), lambda i: (chunk, i))] + [pl.BlockSpec(memory_space=pl.ANY)] * (len(given) + 1),
        jax.ShapeDtypeStruct((2 * tp_size, half, dim), jnp.bfloat16), pl.BlockSpec(memory_space=pl.ANY),
        [
            pltpu.VMEM((cp_size * span, HEAD_DIM), jnp.bfloat16),
            pltpu.VMEM((cp_size * span, HEAD_DIM), jnp.bfloat16),
            pltpu.VMEM((heads, rows, 128), jnp.float32),
            pltpu.VMEM((heads, rows, 128), jnp.float32),
            pltpu.VMEM((heads, rows, HEAD_DIM), jnp.float32),
            pltpu.SemaphoreType.DMA((16,)),
            pltpu.VMEM((rows, depth), jnp.bfloat16),
            pltpu.VMEM((depth, dim), jnp.bfloat16),
            pltpu.VMEM((2 * tp_size, half, dim), jnp.bfloat16),
            pltpu.SemaphoreType.DMA,
            pltpu.SemaphoreType.DMA((n_cols,)),
        ],
        (kv_heads,), 4 * rows * q_cols * kv_heads * span * cp_size + 2 * rows * depth * dim,
        4 * kv_heads * cp_size * span * HEAD_DIM + 2 * depth * dim)


def store_pieces(value, ref):
    pieces, half, unused = ref.shape
    for n in range(pieces):
        ref[n] = value[n * half:(n + 1) * half].astype(jnp.bfloat16)


def mlp(pieces, w_gate, w_up, w_down, tile, ring):
    n_pieces, half, dim = pieces.shape
    rows = n_pieces * half
    width = w_gate.shape[1]
    n_up, n_down = width // tile, dim // tile

    def kernel(ins, out_ref, scratch, ring):
        (pieces_ref, gate_ref, up_ref, down_ref), (act, normed_ref, row_sem) = ins, scratch
        g = pl.program_id(0)
        for step, at in enumerate((0, 2, 4, 6, 8, 9, 12)):
            pl.when(g == at)(ring.steps[step])

        @pl.when(g == 0)
        def _():
            rows_copy = pltpu.make_async_copy(pieces_ref, normed_ref, row_sem)
            rows_copy.start()
            rows_copy.wait()

        @pl.when(g < n_up)
        def _():
            gate = jnp.dot(normed_ref[...], gate_ref[...], preferred_element_type=jnp.float32)
            up = jnp.dot(normed_ref[...], up_ref[...], preferred_element_type=jnp.float32)
            act[:, pl.ds(pl.multiple_of(g * tile, tile), tile)] = (jax.nn.silu(gate) * up).astype(jnp.bfloat16)

        @pl.when(g >= n_up)
        def _():
            store_pieces(jnp.dot(act[...], down_ref[...], preferred_element_type=jnp.float32), out_ref)

        pl.when(g == n_up + n_down - 1)(ring.finish)

    up_spec = pl.BlockSpec((dim, tile), lambda i: (0, jnp.minimum(i, n_up - 1)))
    return host(
        kernel, ring, [pieces.reshape(rows, dim), w_gate, w_up, w_down],
        [pl.BlockSpec(memory_space=pl.ANY), up_spec, up_spec,
         pl.BlockSpec((width, tile), lambda i: (0, jnp.maximum(i - n_up, 0)))],
        jax.ShapeDtypeStruct((n_pieces, half, dim), jnp.bfloat16), pl.BlockSpec((n_pieces, half, tile), lambda i: (0, 0, jnp.maximum(i - n_up, 0))),
        [pltpu.VMEM((rows, width), jnp.bfloat16), pltpu.VMEM((rows, dim), jnp.bfloat16), pltpu.SemaphoreType.DMA], (n_up + n_down,), 6 * rows * dim * width, 6 * dim * width + 6 * rows * dim)


def all_reduce(ring):
    def body(*refs):
        n_in, n_out = len(ring.operands), len(ring.out_shape)
        ring.bind(refs[:n_in], refs[n_in:n_in + n_out], refs[n_in + n_out:])
        for step in (0, 1, 2, 3, 4, 5, 6, 7):
            ring.steps[step]()

    return pl.pallas_call(body, out_shape=ring.out_shape, in_specs=ring.in_specs, out_specs=ring.out_specs, scratch_shapes=ring.scratch,
                          compiler_params=params(ring))(*ring.operands)


def assemble(chunks, axis, size):
    n_pieces, half, dim = chunks[0].shape
    total = len(chunks) * n_pieces

    def kernel(*refs):
        ins, (out_ref, buf, in_sem, out_sem) = refs[:len(chunks)], refs[len(chunks):]
        index = lax.axis_index(axis)
        places = []
        for n in range(total):
            step = (0, size - 1, 1, 2)[n % n_pieces // 2]
            start = (n // n_pieces * n_pieces + n % 2 + 2 * lax.rem(index + step, size)) * half
            places.append(pl.ds(pl.multiple_of(start, half), half))
        loads = [pltpu.make_async_copy(ins[n // n_pieces].at[n % n_pieces], buf.at[n], in_sem.at[n]) for n in range(total)]
        stores = [pltpu.make_async_copy(buf.at[n], out_ref.at[places[n]], out_sem.at[n]) for n in range(total)]
        for load in loads:
            load.start()
        for load, store in zip(loads, stores):
            load.wait()
            store.start()
        for store in stores:
            store.wait()

    return pl.pallas_call(
        kernel,
        out_shape=jax.ShapeDtypeStruct((total * half, dim), jnp.bfloat16),
        in_specs=[pl.BlockSpec(memory_space=pl.ANY)] * len(chunks),
        out_specs=pl.BlockSpec(memory_space=pl.ANY),
        scratch_shapes=[pltpu.VMEM((total, half, dim), jnp.bfloat16), pltpu.SemaphoreType.DMA((total,)), pltpu.SemaphoreType.DMA((total,))],
        compiler_params=pltpu.CompilerParams(vmem_limit_bytes=VMEM_LIMIT),
        cost_estimate=pl.CostEstimate(flops=0, bytes_accessed=4 * total * half * dim, transcendentals=0),
    )(*chunks)


def solution(mesh):
    cp_size = mesh.shape['cp']
    tp_size = mesh.shape['tp']
    row_spec = P(('dp', 'cp'), None)
    cache_spec = P(('dp', 'cp'), 'tp', None)
    col_spec = P(None, 'tp')
    split_rows = P('tp', None)
    vec_spec = P(None)

    def local_layer(x, attn_gain, w_q, w_k, w_v, w_o, mlp_gain, w_gate, w_up, w_down):
        tok_dev = x.shape[0]
        kv_local = w_k.shape[1] // HEAD_DIM
        kv_cols = w_k.shape[1]
        cp_index = lax.axis_index('cp')
        cos_tab, sin_tab = rope_tables(cp_index * tok_dev + jnp.arange(tok_dev))
        block = (tok_dev, 2 * kv_cols)
        queries, low, high, mate, own = project(x, attn_gain, cos_tab, sin_tab, w_k, w_v, w_q, Links('cp', cp_size, [], block, 4, 4))
        blocks = [own, low, None, high, mate, None, None, None]
        rows = tok_dev // 2

        def attend(chunk, ring=None):
            return attention(queries, blocks, w_o, chunk, rows, kv_local, 'cp', cp_size, 'tp', tp_size, ring)

        def reduce_over_tp(partial, base, base_row, gain, ring_id):
            return Ring('tp', tp_size, partial, base, base_row, gain, ring_id)

        part0, far, mate_low, mate_far, mate_high = attend(0, Links('cp', cp_size, [low, high], block, 4, 5))
        blocks = [own, low, far, high, mate, mate_low, mate_far, mate_high]
        part1, normed0, hidden0 = attend(1, reduce_over_tp(part0, x, 0, mlp_gain, 0))
        down0, normed1, hidden1 = mlp(normed0, w_gate, w_up, w_down, FF_TILE, reduce_over_tp(part1, x, rows, mlp_gain, 1))
        down1, out0 = mlp(normed1, w_gate, w_up, w_down, FF_TILE, reduce_over_tp(down0, hidden0, None, None, 2))
        out1 = all_reduce(reduce_over_tp(down1, hidden1, None, None, 3))[0]
        x_out = assemble([out0, out1], 'tp', tp_size)
        cache_shape = (tok_dev, kv_local, HEAD_DIM)
        return x_out, own[:, :kv_cols].reshape(cache_shape), own[:, kv_cols:].reshape(cache_shape)

    return jax.shard_map(local_layer, mesh=mesh,
                         in_specs=(row_spec, vec_spec, col_spec, col_spec, col_spec, split_rows, vec_spec, col_spec, col_spec, split_rows),
                         out_specs=(row_spec, cache_spec, cache_spec), check_vma=False)
```
